256 devices in a mesh: tile: 32 (over y, z), cplx: 8 (over x, core).
Axes of the slice: x: 4, y: 4, z: 8, core: 2. Of those that a mesh axis runs over, the one named last changes fastest.
Arguments:
- pair_tiles: bfloat16 [768, 128, 128, 128], P(('tile', 'cplx'))
- tile_map: int32 [768, 3], replicated, may hold values from -1 to 47, as said below
- lengths: int32 [48], replicated, may hold values from 256 to 512
- resolved: int32 [48, 512], replicated, may hold values 0 or 1
- ln_gain: float32 [128], replicated, may hold values from 0.1 to 1.9
- w_in: bfloat16 [128, 512], replicated, may hold values from -0.5 to 0.5
- w_out: bfloat16 [512, 128], replicated, may hold values from -0.25 to 0.25
- w_head: bfloat16 [128, 64], replicated
- head_bias: float32 [64], replicated, may hold values from -4 to 4
Outputs:
- error_map: float32 [48, 512, 512], P('cplx', 'tile')
- residue_error: float32 [48, 512], P('cplx', 'tile')
- tm_score: float32 [48], P('cplx')
The draws below stay inside these ranges and needn't reach their ends.
Inputs may be any that keep to these rules, and one draw needn't show every extreme that they name: `tile_map`: row (t * 8 + c) * 3 + j is slot j of the device at tile index t and cplx index c and holds the complex, block row and block column of its tile, or -1 three times where the slot is empty. Each tile (k, r, q) with r and q below ceil(lengths[k] / 128) is held by exactly one slot and no other tile is held. Complex k is owned by cplx index k // 6; no two filled slots of one device have the same owner, and for fixed t and j the owners over the 8 cplx indices are all different.
All inputs are finite; a program needn't handle non-finite values.
Results may differ from the reference program's by a relative error of at most 0.0089.
Values sent between devices are 32-bit elements; how exact they have to be, the bound alone decides.
A program may use at most 128 MiB of HBM per device.

```python
import math
import jax
import jax.numpy as jnp
from jax import lax

C = 128
HID = 512
BINS = 64
TILE = 128
BLOCKS = 4
TILES_DEV = 3
MAXRES = 512
COMPLEXES = 48
TILES = 768
N_TILE = 32
N_CPLX = 8


def draw_pair_tiles(key, part):
    shape = (TILES, TILE, TILE, C)
    base = jax.random.normal(jax.random.fold_in(key, 3), shape, jnp.float32)
    top_scale = math.sqrt(10.0)
    row_scale = jnp.exp(jax.random.uniform(jax.random.fold_in(key, 5), (TILES, TILE, 1, 1), jnp.float32, 0.0, math.log(top_scale)))
    col_scale = jnp.exp(jax.random.uniform(jax.random.fold_in(key, 7), (TILES, 1, TILE, 1), jnp.float32, 0.0, math.log(top_scale)))
    return (base * row_scale * col_scale).astype(jnp.bfloat16)


def draw_w_head(key, part):
    base = jax.random.normal(jax.random.fold_in(key, 9), (C, BINS), jnp.float32)
    return (base * (3.0 / math.sqrt(C))).astype(jnp.bfloat16)


def complex_lengths(key):
    drawn = jax.random.randint(jax.random.fold_in(key, 17), (COMPLEXES,), MAXRES // 2, MAXRES + 1).astype(jnp.int32)
    longest = jax.random.randint(jax.random.fold_in(key, 19), (), 0, COMPLEXES).astype(jnp.int32)
    shortest = (longest + 1) % COMPLEXES
    drawn = drawn.at[shortest].set(MAXRES // 2)
    drawn = drawn.at[longest].set(MAXRES)
    return drawn.astype(jnp.int32)


def draw_lengths(key, part):
    return complex_lengths(key)


def draw_tile_map(key, part):
    lengths = complex_lengths(key)
    block_counts = (lengths + TILE - 1) // TILE
    cpx_dev = COMPLEXES // N_CPLX
    per_owner = N_TILE * TILES_DEV
    row_keys = jax.random.split(jax.random.fold_in(key, 29), N_TILE)
    offsets = jax.vmap(lambda sub_key: jax.random.permutation(sub_key, N_CPLX))(row_keys)[:, :TILES_DEV]
    owner_keys = jax.random.split(jax.random.fold_in(key, 31), N_CPLX)
    owner_ranks = jax.vmap(lambda sub_key: jax.random.permutation(sub_key, per_owner))(owner_keys)
    local_index = jnp.arange(cpx_dev * BLOCKS * BLOCKS, dtype=jnp.int32)
    member = local_index // (BLOCKS * BLOCKS)
    block_row = local_index // BLOCKS % BLOCKS
    block_col = local_index % BLOCKS
    owners = jnp.arange(N_CPLX, dtype=jnp.int32)
    complex_id = owners[:, None] * cpx_dev + member[None, :]
    block_count = block_counts[complex_id]
    is_live = (block_row[None, :] < block_count) & (block_col[None, :] < block_count)
    position = jnp.cumsum(is_live.astype(jnp.int32), axis=1) - 1
    tile_table = jnp.full((N_CPLX, per_owner), -1, jnp.int32)
    tile_table = tile_table.at[jnp.broadcast_to(owners[:, None], is_live.shape), jnp.where(is_live, position, per_owner)].set(jnp.broadcast_to(local_index[None, :], is_live.shape), mode='drop')
    tiles_t = jnp.arange(N_TILE, dtype=jnp.int32)[:, None, None]
    cplx_ids = jnp.arange(N_CPLX, dtype=jnp.int32)[None, :, None]
    slot_ids = jnp.arange(TILES_DEV, dtype=jnp.int32)[None, None, :]
    owner_of = (cplx_ids + offsets[:, None, :]) % N_CPLX
    rank_of = owner_ranks[owner_of, tiles_t * TILES_DEV + slot_ids]
    chosen = tile_table[owner_of, rank_of]
    filled = chosen >= 0
    safe_pick = jnp.maximum(chosen, 0)
    result = jnp.stack([jnp.where(filled, owner_of * cpx_dev + safe_pick // (BLOCKS * BLOCKS), -1), jnp.where(filled, safe_pick // BLOCKS % BLOCKS, -1), jnp.where(filled, safe_pick % BLOCKS, -1)], axis=-1)
    return result.reshape(N_TILE * N_CPLX * TILES_DEV, 3).astype(jnp.int32)


def set_ends(values, stream_key, smallest, top_value):
    longest = values.shape.index(max(values.shape))
    spots = []
    for shift in (0, 1):
        where = [jax.random.randint(jax.random.fold_in(stream_key, axis), (), 0, length) for axis, length in enumerate(values.shape)]
        where[longest] = (where[longest] + shift) % values.shape[longest]
        spots.append(tuple(where))
    return values.at[spots[0]].set(smallest).at[spots[1]].set(top_value)


def bell_draw(rng, shape, width, limit, kind=jnp.bfloat16):
    array = width * jax.random.normal(rng, shape, jnp.float32)
    return jnp.clip(array, min=-limit, max=limit).astype(kind)


def setup_inputs(seed: int = 0) -> dict:
    streams_of = jax.random.split(jax.random.key(seed), 10)
    return {
        "pair_tiles": draw_pair_tiles(jax.random.fold_in(streams_of[9], 71), 0),
        "tile_map": draw_tile_map(jax.random.fold_in(streams_of[9], 71), 0),
        "lengths": draw_lengths(jax.random.fold_in(streams_of[9], 71), 0),
        "resolved": set_ends((jax.random.randint(streams_of[3], (COMPLEXES, MAXRES), 0, 8) < 7).astype(jnp.int32), jax.random.fold_in(streams_of[3], 1), 0, 1),
        "ln_gain": jnp.clip(1.0 + 0.18 * jax.random.normal(streams_of[4], (C,), jnp.float32), 0.1, 1.9),
        "w_in": bell_draw(streams_of[5], (C, HID), C ** -0.5, 0.5),
        "w_out": bell_draw(streams_of[6], (HID, C), HID ** -0.5, 0.25),
        "w_head": draw_w_head(jax.random.fold_in(streams_of[9], 71), 0),
        "head_bias": bell_draw(streams_of[8], (BINS,), 1.0, 4.0, jnp.float32),
    }


EPS = 1e-05

def bin_centers(bin_count):
    bin_step = 31.0 / (bin_count - 2)
    return (jnp.arange(bin_count, dtype=jnp.float32) + 0.5) * bin_step

def d_zero(length):
    clipped = jnp.maximum(length, 19).astype(jnp.float32)
    return 1.24 * jnp.cbrt(clipped - 15.0) - 1.8

def pair_head(row_block, ln_gain, w_in, w_out, w_head, head_bias, centers, distance):
    values = row_block.astype(jnp.float32)
    row_mean = lax.optimization_barrier(jnp.mean(values, axis=-1, keepdims=True))
    centred = values - row_mean
    variance = lax.optimization_barrier(jnp.mean(centred * centred, axis=-1, keepdims=True))
    normed = (centred * lax.rsqrt(variance + EPS) * ln_gain).astype(jnp.bfloat16)
    hidden = jax.nn.relu(jnp.dot(normed, w_in, preferred_element_type=jnp.float32)).astype(jnp.bfloat16)
    updated = (values + jnp.dot(hidden, w_out, preferred_element_type=jnp.float32)).astype(jnp.bfloat16)
    logits = jnp.dot(updated, w_head, preferred_element_type=jnp.float32) + head_bias
    bin_probs = jax.nn.softmax(logits, axis=-1)
    expected = lax.optimization_barrier(jnp.sum(bin_probs * centers, axis=-1))
    tm_term = lax.optimization_barrier(jnp.sum(bin_probs / (1.0 + (centers / distance) ** 2), axis=-1))
    return (expected, tm_term)

def reference(pair_tiles, tile_map, lengths, resolved, ln_gain, w_in, w_out, w_head, head_bias):
    centers = bin_centers(BINS)
    positions = jnp.arange(MAXRES, dtype=jnp.int32)
    valid_mask = ((positions[None, :] < lengths[:, None]) & (resolved > 0)).astype(jnp.float32)

    def visit_slot(carry_state, slot_item):
        error_map, score_rows = carry_state
        one_tile, slot_meta = slot_item
        present = slot_meta[0] >= 0
        complex_id = jnp.maximum(slot_meta[0], 0).astype(jnp.int32)
        block_row = jnp.maximum(slot_meta[1], 0).astype(jnp.int32)
        block_col = jnp.maximum(slot_meta[2], 0).astype(jnp.int32)
        distance = d_zero(lengths[complex_id])
        expected, tm_term = pair_head(one_tile.reshape(TILE * TILE, C), ln_gain, w_in, w_out, w_head, head_bias, centers, distance)
        row_valid = lax.dynamic_slice(valid_mask, (complex_id, block_row * TILE), (1, TILE))[0]
        col_valid = lax.dynamic_slice(valid_mask, (complex_id, block_col * TILE), (1, TILE))[0]
        weight = jnp.where(present, row_valid[:, None] * col_valid[None, :], jnp.float32(0.0))
        error_tile = weight * expected.reshape(TILE, TILE)
        score_tile = lax.optimization_barrier(jnp.sum(weight * tm_term.reshape(TILE, TILE), axis=1))
        corner = (complex_id, block_row * TILE, block_col * TILE)
        previous = lax.dynamic_slice(error_map, corner, (1, TILE, TILE))
        error_map = lax.dynamic_update_slice(error_map, previous + error_tile[None], corner)
        row_corner = (complex_id, block_row * TILE)
        previous_rows = lax.dynamic_slice(score_rows, row_corner, (1, TILE))
        score_rows = lax.dynamic_update_slice(score_rows, previous_rows + score_tile[None], row_corner)
        return ((error_map, score_rows), None)
    initial = (jnp.zeros((COMPLEXES, MAXRES, MAXRES), jnp.float32), jnp.zeros((COMPLEXES, MAXRES), jnp.float32))
    (error_map, score_rows), _ = lax.scan(visit_slot, initial, (pair_tiles, tile_map))
    denominator = jnp.maximum(valid_mask * lax.optimization_barrier(jnp.sum(valid_mask, axis=1, keepdims=True)), jnp.float32(1.0))
    residue_error = lax.optimization_barrier(jnp.sum(error_map, axis=2)) / denominator
    tm_score = lax.optimization_barrier(jnp.max(score_rows / denominator, axis=1))
    return (error_map, residue_error, tm_score)
```

```python
import functools
import jax
import jax.numpy as jnp
from jax import lax
from jax.experimental import pallas as pl
from jax.experimental.pallas import tpu as pltpu
from jax.sharding import PartitionSpec as P

EPS = 1e-05
LOG2E = 1.4426950408889634
F32 = jnp.float32
BF16 = jnp.bfloat16


def head_kernel(
    slots_ref,
    lengths_ref,
    x_ref,
    resolved_ref,
    gain_ref,
    w_in_ref,
    w_out_ref,
    w_head_ref,
    bias_ref,
    err_ref,
    tm_ref,
    mix_s,
    w1_s,
    w2_s,
    bias_s,
    cen_s,
    tmw_s,
    tmt_s,
    *,
    rows,
    group,
):
    slot = pl.program_id(0)
    step = pl.program_id(1)
    side = x_ref.shape[2]
    chan = x_ref.shape[3]
    bins = w_head_ref.shape[1]
    lanes = 128

    @pl.when((slot == 0) & (step == 0))
    def _():
        r = lax.broadcasted_iota(jnp.int32, (chan, chan), 0)
        c = lax.broadcasted_iota(jnp.int32, (chan, chan), 1)
        mix_s[0:chan, :] = (jnp.where(r == c, 1.0, 0.0) - 1.0 / chan).astype(BF16)
        mix_s[chan : chan + bins, :] = w_head_ref[...].astype(F32).T.astype(BF16)
        w1_s[...] = (w_in_ref[...].astype(F32).T * gain_ref[...]).astype(BF16)
        w2_s[...] = lax.dot_general(
            w_head_ref[...],
            w_out_ref[...],
            (((0,), (1,)), ((), ())),
            preferred_element_type=F32,
        ).astype(BF16)
        bias_s[...] = jnp.broadcast_to(bias_ref[...], (lanes, bins)).T
        b = lax.broadcasted_iota(jnp.int32, (bins, lanes), 0).astype(F32)
        cen_s[...] = (b + 0.5) * (31.0 / (bins - 2))

    k = jnp.maximum(slots_ref[slot, 0], 0)
    length = lengths_ref[k]

    @pl.when(step == 0)
    def _():
        size = jnp.full((bins, lanes), jnp.maximum(length, 19).astype(F32) - 15.0, F32)
        d0 = 1.24 * jnp.exp(jnp.log(size) * (1.0 / 3.0)) - 1.8
        ratio = cen_s[...] / d0
        tmw_s[...] = 1.0 / (1.0 + ratio * ratio)

    present = slots_ref[slot, 0] >= 0

    @pl.when(present)
    def _():
        cen = jnp.concatenate([cen_s[...]] * group, axis=1)
        tmw = jnp.concatenate([tmw_s[...]] * group, axis=1)
        bias = jnp.concatenate([bias_s[...]] * group, axis=1)

        def body(g, carry):
            row = pl.multiple_of(g * group, group)
            x = x_ref[0, pl.ds(row, group), :, :].reshape(group * side, chan)
            first = lax.dot_general(
                mix_s[...], x, (((1,), (1,)), ((), ())), preferred_element_type=F32
            )
            xc = first[:chan]
            var = jnp.mean(xc * xc, axis=0, keepdims=True)
            rstd = lax.rsqrt(var + EPS)
            z = jnp.dot(w1_s[...], xc.astype(BF16), preferred_element_type=F32)
            h = jnp.maximum(z, 0.0).astype(BF16)
            y = jnp.dot(w2_s[...], h, preferred_element_type=F32)
            logits = (first[chan:] + rstd * y + bias) * LOG2E
            top = jnp.max(logits, axis=0, keepdims=True)
            p = jnp.exp2(logits - top)
            s0 = jnp.sum(p, axis=0, keepdims=True)
            s1 = jnp.sum(p * cen, axis=0, keepdims=True)
            s2 = jnp.sum(p * tmw, axis=0, keepdims=True)
            inv = 1.0 / s0
            expected = s1 * inv
            term = s2 * inv
            at = step * rows + row
            for i in range(group):
                err_ref[0, pl.ds(at + i, 1), :] = expected[:, i * side : (i + 1) * side]
                tmt_s[pl.ds(at + i, 1), :] = term[:, i * side : (i + 1) * side]
            return carry

        lax.fori_loop(0, rows // group, body, 0)

    @pl.when(step == pl.num_programs(1) - 1)
    def _():
        @pl.when(present)
        def _():
            br = jnp.maximum(slots_ref[slot, 1], 0)
            bc = jnp.maximum(slots_ref[slot, 2], 0)
            pos = lax.broadcasted_iota(jnp.int32, (1, side), 1)

            def valid(block):
                line = resolved_ref[pl.ds(k, 1), :]
                res = jnp.zeros((1, side), jnp.int32)
                for b in range(line.shape[1] // side):
                    res = jnp.where(block == b, line[:, b * side : (b + 1) * side], res)
                return jnp.where((pos + block * side < length) & (res > 0), 1.0, 0.0)

            row_valid = jnp.broadcast_to(valid(br), (side, side)).T
            weight = row_valid * valid(bc)
            err_ref[0] = err_ref[0] * weight
            tm_ref[0] = jnp.sum((tmt_s[...] * weight).T, axis=0, keepdims=True)

        @pl.when(jnp.logical_not(present))
        def _():
            err_ref[...] = jnp.zeros_like(err_ref)
            tm_ref[...] = jnp.zeros_like(tm_ref)


def head(pair_tiles, own_slots, lengths, resolved, ln_gain, w_in, w_out, w_head, head_bias, rows=32, group=4):
    slots, side, _, chan = pair_tiles.shape
    hid = w_in.shape[1]
    bins = w_head.shape[1]

    def whole(*shape):
        return pl.BlockSpec(shape, lambda s, i, *_: (0,) * len(shape))

    return pl.pallas_call(
        functools.partial(head_kernel, rows=rows, group=group),
        grid_spec=pltpu.PrefetchScalarGridSpec(
            num_scalar_prefetch=2,
            grid=(slots, side // rows),
            in_specs=[
                pl.BlockSpec((1, rows, side, chan), lambda s, i, *_: (s, i, 0, 0)),
                whole(*resolved.shape),
                whole(1, chan),
                whole(chan, hid),
                whole(hid, chan),
                whole(chan, bins),
                whole(1, bins),
            ],
            out_specs=[
                pl.BlockSpec((1, side, side), lambda s, i, *_: (s, 0, 0)),
                pl.BlockSpec((1, 1, side), lambda s, i, *_: (s, 0, 0)),
            ],
            scratch_shapes=[
                pltpu.VMEM((chan + bins, chan), BF16),
                pltpu.VMEM((hid, chan), BF16),
                pltpu.VMEM((bins, hid), BF16),
                pltpu.VMEM((bins, 128), F32),
                pltpu.VMEM((bins, 128), F32),
                pltpu.VMEM((bins, 128), F32),
                pltpu.VMEM((side, side), F32),
            ],
        ),
        out_shape=[
            jax.ShapeDtypeStruct((slots, side, side), F32),
            jax.ShapeDtypeStruct((slots, 1, side), F32),
        ],
        compiler_params=pltpu.CompilerParams(
            dimension_semantics=("arbitrary", "arbitrary"),
            vmem_limit_bytes=48 * 1024 * 1024,
        ),
        name="head",
    )(
        own_slots,
        lengths,
        pair_tiles,
        resolved,
        ln_gain.reshape(1, chan),
        w_in,
        w_out,
        w_head,
        head_bias.reshape(1, bins),
    )


def in_one_piece(arrays, axis, split_dim, concat_dim, along):
    columns = [a.reshape(*a.shape[:along], -1) for a in arrays]
    both = jnp.concatenate(columns, axis=along)
    out, at, finished = (
        lax.all_to_all(both, axis, split_axis=split_dim, concat_axis=concat_dim, tiled=True),
        0,
        [],
    )
    for a, column in zip(arrays, columns):
        section = out[..., at : at + column.shape[along]]
        finished.append(section.reshape(*section.shape[:along], *a.shape[along:]))
        at += column.shape[along]
    return tuple(finished)


def copy_for_each(array, axis):
    copies = jnp.broadcast_to(array, (lax.axis_size(axis), *array.shape))
    return lax.all_to_all(copies, axis, split_axis=0, concat_axis=0, tiled=True)


def taken_together(array, axis):
    everything = copy_for_each(array, axis)
    return jnp.max(everything, axis=0)


def route_rows(
    error_src, rows_src, row_src, found_src, n_tile, parts_per, rows_each, tile_side, highest
):
    target_rows = jnp.arange(n_tile, dtype=jnp.int32)[:, None, None]
    part_index = jnp.arange(parts_per, dtype=jnp.int32)[None, None, :]
    routing = (
        (target_rows == row_src[None, :, None] * parts_per + part_index) & found_src[None, :, None]
    ).astype(jnp.float32)
    sender_count = error_src.shape[0]
    error_parts = error_src.reshape(sender_count, parts_per, rows_each, tile_side)
    row_parts = rows_src.reshape(sender_count, parts_per, rows_each)
    error_out = jnp.einsum("tcq,cqrj->tcrj", routing, error_parts, precision=highest)
    rows_out = jnp.einsum("tcq,cqr->tcr", routing, row_parts, precision=highest)
    return (error_out, rows_out)


def place_rows(
    error_back,
    rows_back,
    member_all,
    row_all,
    colblk_all,
    found_all,
    row_index,
    parts_per,
    cpx_dev,
    blocks,
    rows_each,
    tile_side,
    maxres,
    highest,
):
    mine_rows = found_all & (row_all == row_index // parts_per)
    member_hot = (
        (jnp.arange(cpx_dev, dtype=jnp.int32)[None, None, :] == member_all[..., None])
        & mine_rows[..., None]
    ).astype(jnp.float32)
    block_hot = (
        jnp.arange(blocks, dtype=jnp.int32)[None, None, :] == colblk_all[..., None]
    ).astype(jnp.float32)
    sources = member_all.shape[0] * member_all.shape[1]
    place_hot = (member_hot[..., :, None] * block_hot[..., None, :]).reshape(
        sources, cpx_dev, blocks
    )
    share_map = jnp.einsum(
        "smb,srj->mrbj",
        place_hot,
        error_back.reshape(sources, rows_each, tile_side),
        precision=highest,
    ).reshape(cpx_dev, rows_each, maxres)
    share_rows = jnp.einsum(
        "sm,sr->mr",
        member_hot.reshape(sources, cpx_dev),
        rows_back.reshape(sources, rows_each),
        precision=highest,
    )
    return (share_map, share_rows)


def shards(pair_tiles, tile_map, lengths, resolved, ln_gain, w_in, w_out, w_head, head_bias):
    highest = lax.Precision.HIGHEST
    n_tile = lax.axis_size("tile")
    n_cplx = lax.axis_size("cplx")
    row_index = lax.axis_index("tile")
    col_index = lax.axis_index("cplx")
    slot_count, tile_side = pair_tiles.shape[:2]
    complexes, maxres = resolved.shape
    blocks = maxres // tile_side
    cpx_dev = complexes // n_cplx
    rows_each = maxres // n_tile
    parts_per = tile_side // rows_each
    positions = jnp.arange(maxres, dtype=jnp.int32)
    valid_mask = ((positions[None, :] < lengths[:, None]) & (resolved > 0)).astype(jnp.float32)
    layout = tile_map.reshape(n_tile, n_cplx, slot_count, 3)
    own_slots = layout[row_index, col_index]
    error_tiles, score_rows = head(
        pair_tiles, own_slots, lengths, resolved, ln_gain, w_in, w_out, w_head, head_bias
    )
    score_rows = score_rows[:, 0]
    owner_ids = jnp.where(own_slots[:, 0] >= 0, own_slots[:, 0] // cpx_dev, -1)
    select = (jnp.arange(n_cplx, dtype=jnp.int32)[:, None] == owner_ids[None, :]).astype(
        jnp.float32
    )
    error_send = jnp.einsum("os,sij->oij", select, error_tiles, precision=highest)
    score_send = jnp.einsum("os,si->oi", select, score_rows, precision=highest)
    error_in, rows_in = in_one_piece((error_send, score_send), "cplx", 0, 0, 2)
    complex_all = layout[..., 0]
    owner_all = jnp.where(complex_all >= 0, complex_all // cpx_dev, -1)
    matched = owner_all == col_index
    matched_float = matched.astype(jnp.float32)
    slot_hot = matched_float[row_index]
    error_slots = jnp.einsum("sj,sab->jab", slot_hot, error_in, precision=highest)
    rows_slots = jnp.einsum("sj,sa->ja", slot_hot, rows_in, precision=highest)
    found_slot = jnp.any(matched, axis=1)

    def pick_slot(column):
        return jnp.sum(jnp.where(matched, layout[..., column], 0), axis=1)

    member_slot = pick_slot(0) - col_index * cpx_dev
    row_slot = pick_slot(1)
    colblk_slot = pick_slot(2)
    error_out, rows_out = route_rows(
        error_slots,
        rows_slots,
        row_slot[row_index],
        found_slot[row_index],
        n_tile,
        parts_per,
        rows_each,
        tile_side,
        highest,
    )
    error_back, rows_back = (
        lax.all_to_all(error_out, "tile", split_axis=0, concat_axis=0, tiled=True),
        lax.all_to_all(rows_out, "tile", split_axis=0, concat_axis=0, tiled=True),
    )
    share_map, share_rows = place_rows(
        error_back,
        rows_back,
        member_slot,
        row_slot,
        colblk_slot,
        found_slot,
        row_index,
        parts_per,
        cpx_dev,
        blocks,
        rows_each,
        tile_side,
        maxres,
        highest,
    )
    valid_rows = lax.dynamic_slice(
        valid_mask, (col_index * cpx_dev, row_index * rows_each), (cpx_dev, rows_each)
    )
    totals = lax.dynamic_slice_in_dim(jnp.sum(valid_mask, axis=1), col_index * cpx_dev, cpx_dev)
    denominator = jnp.maximum(valid_rows * totals[:, None], jnp.float32(1.0))
    residue_error = jnp.sum(share_map, axis=2) / denominator
    best_share = jnp.max(share_rows / denominator, axis=1)
    tm_score = taken_together(best_share, "tile")
    return (share_map, residue_error, tm_score)


def solution(mesh):
    placed = (P(("tile", "cplx"), None, None, None), P(), P(), P(), P(), P(), P(), P(), P())
    return jax.shard_map(
        shards,
        mesh=mesh,
        in_specs=placed,
        out_specs=(P("cplx", "tile", None), P("cplx", "tile"), P("cplx")),
        check_vma=False,
    )
```

```python
import functools
import jax
import jax.numpy as jnp
from jax import lax
from jax.experimental import pallas as pl
from jax.experimental.pallas import tpu as pltpu
from jax.sharding import PartitionSpec as P

EPS = 1e-05
LOG2E = 1.4426950408889634
F32 = jnp.float32
BF16 = jnp.bfloat16
MESH = pl.DeviceIdType.MESH
GROUP = 4


def fused_kernel(
    table_ref,
    lengths_ref,
    x_ref,
    resolved_ref,
    gain_ref,
    w_in_ref,
    w_out_ref,
    w_head_ref,
    bias_ref,
    map_ref,
    res_ref,
    best_ref,
    mix_s,
    w1_s,
    w2_s,
    bias_s,
    cen_s,
    tmw_s,
    weight_s,
    x_s,
    err_s,
    tm_s,
    send_s,
    sendt_s,
    recv_s,
    recvt_s,
    ysend_s,
    ysendt_s,
    yrecv_s,
    yrecvt_s,
    top_s,
    topz_s,
    topy_s,
    x_sem,
    send_sem,
    sendt_sem,
    recv_sem,
    recvt_sem,
    ysend_sem,
    yrecv_sem,
    yrecvt_sem,
    topsend_sem,
    topz_sem,
    topy_sem,
    *,
    blocks,
    parts,
    n_cplx,
):
    slots, side, _, chan = x_ref.shape
    bins = w_head_ref.shape[1]
    lanes = 128
    rows = side // parts
    cpx_dev = map_ref.shape[0]
    cells = cpx_dev * blocks
    tile = lax.axis_index("tile")
    mine = lax.axis_index("cplx")
    by = tile // parts
    bz = lax.rem(tile, parts)

    def x_copy(s, j):
        p = lax.rem(bz + parts - 1 - s, parts)
        at = lax.rem(s, 2)
        return pltpu.make_async_copy(
            x_ref.at[j, pl.ds(p * rows, rows)],
            x_s.at[at, pl.ds(j * rows, rows)],
            x_sem.at[at, j],
        )

    for j in range(slots):
        x_copy(0, j).start()

    barrier = pltpu.get_barrier_semaphore()
    plane = parts * n_cplx

    def greet(d, carry):
        other = lax.rem(bz * n_cplx + mine + d, plane)
        pl.semaphore_signal(
            barrier,
            inc=1,
            device_id=(by * parts + other // n_cplx, lax.rem(other, n_cplx)),
            device_id_type=MESH,
        )
        return carry

    lax.fori_loop(1, plane, greet, 0)
    for d in range(1, blocks):
        pl.semaphore_signal(
            barrier,
            inc=1,
            device_id=(lax.rem(by + d, blocks) * parts + bz, mine),
            device_id_type=MESH,
        )

    r = lax.broadcasted_iota(jnp.int32, (chan, chan), 0)
    c = lax.broadcasted_iota(jnp.int32, (chan, chan), 1)
    mix_s[0:chan, :] = (jnp.where(r == c, 1.0, 0.0) - 1.0 / chan).astype(BF16)
    mix_s[chan : chan + bins, :] = w_head_ref[...].astype(F32).T.astype(BF16)
    w1_s[...] = (w_in_ref[...].astype(F32).T * gain_ref[...]).astype(BF16)
    w2_s[...] = lax.dot_general(
        w_head_ref[...], w_out_ref[...], (((0,), (1,)), ((), ())), preferred_element_type=F32
    ).astype(BF16)
    bias_s[...] = jnp.broadcast_to(bias_ref[...], (lanes, bins)).T
    b = lax.broadcasted_iota(jnp.int32, (bins, lanes), 0).astype(F32)
    cen_s[...] = (b + 0.5) * (31.0 / (bins - 2))
    pos = lax.broadcasted_iota(jnp.int32, (1, side), 1)

    def valid(k, length, block):
        line = resolved_ref[pl.ds(k, 1), :]
        part = jnp.zeros((1, side), jnp.int32)
        for q in range(blocks):
            part = jnp.where(block == q, line[:, q * side : (q + 1) * side], part)
        return jnp.where((pos + block * side < length) & (part > 0), 1.0, 0.0)

    owners = []
    for j in range(slots):
        found = table_ref[3 * j]
        k = jnp.maximum(found, 0)
        length = lengths_ref[k]
        size = jnp.full((bins, lanes), jnp.maximum(length, 19).astype(F32) - 15.0, F32)
        d0 = 1.24 * jnp.exp(jnp.log(size) * (1.0 / 3.0)) - 1.8
        ratio = cen_s[...] / d0
        tmw_s[j] = 1.0 / (1.0 + ratio * ratio)
        row_valid = valid(k, length, jnp.maximum(table_ref[3 * j + 1], 0))
        col_valid = valid(k, length, jnp.maximum(table_ref[3 * j + 2], 0))
        col_valid = jnp.where(found >= 0, col_valid, 0.0)
        weight_s[j] = jnp.broadcast_to(row_valid, (side, side)).T * col_valid
        owners.append(jnp.where(found >= 0, k // cpx_dev, -1))

    per_slot = rows // GROUP
    tm_s[...] = jnp.zeros_like(tm_s)

    def err_copy(s, d):
        p = lax.rem(bz + parts - 1 - s, parts)
        o = lax.rem(mine + d, n_cplx)
        return pltpu.make_async_remote_copy(
            src_ref=send_s.at[s, o],
            dst_ref=recv_s.at[bz * n_cplx + mine],
            send_sem=send_sem.at[s],
            recv_sem=recv_sem.at[bz],
            device_id=(by * parts + p, o),
            device_id_type=MESH,
        )

    def tm_copy(s, d):
        p = lax.rem(bz + parts - 1 - s, parts)
        o = lax.rem(mine + d, n_cplx)
        return pltpu.make_async_remote_copy(
            src_ref=sendt_s.at[s],
            dst_ref=recvt_s.at[bz * n_cplx + mine],
            send_sem=sendt_sem.at[s],
            recv_sem=recvt_sem.at[bz],
            device_id=(by * parts + p, o),
            device_id_type=MESH,
        )

    def stage(s, carry):
        at = lax.rem(s, 2)

        @pl.when(s < parts - 1)
        def _():
            for j in range(slots):
                x_copy(s + 1, j).start()

        for j in range(slots):
            x_copy(s, j).wait()

        def body(it, inner):
            row = pl.multiple_of(it * GROUP, GROUP)
            slot = it // per_slot
            x = x_s[at, pl.ds(row, GROUP), :, :].reshape(GROUP * side, chan)
            cen = jnp.concatenate([cen_s[...]] * GROUP, axis=1)
            tmw = jnp.concatenate([tmw_s[slot]] * GROUP, axis=1)
            bias = jnp.concatenate([bias_s[...]] * GROUP, axis=1)
            first = lax.dot_general(
                mix_s[...], x, (((1,), (1,)), ((), ())), preferred_element_type=F32
            )
            xc = first[:chan]
            var = jnp.mean(xc * xc, axis=0, keepdims=True)
            rstd = lax.rsqrt(var + EPS)
            z = jnp.dot(w1_s[...], xc.astype(BF16), preferred_element_type=F32)
            h = jnp.maximum(z, 0.0).astype(BF16)
            y = jnp.dot(w2_s[...], h, preferred_element_type=F32)
            logits = (first[chan:] + rstd * y + bias) * LOG2E
            top = jnp.max(logits, axis=0, keepdims=True)
            e = jnp.exp2(logits - top)
            s0 = jnp.sum(e, axis=0, keepdims=True)
            s1 = jnp.sum(e * cen, axis=0, keepdims=True)
            s2 = jnp.sum(e * tmw, axis=0, keepdims=True)
            inv = 1.0 / s0
            expected = s1 * inv
            term = s2 * inv
            for i in range(GROUP):
                err_s[pl.ds(row + i, 1), :] = expected[:, i * side : (i + 1) * side]
                tm_s[pl.ds(row + i, 1), :] = term[:, i * side : (i + 1) * side]
            return inner

        lax.fori_loop(0, slots * per_slot, body, 0)

        p = lax.rem(bz + parts - 1 - s, parts)
        start = pl.multiple_of(p * rows, rows)
        errs = []
        for j in range(slots):
            weight = weight_s[j, pl.ds(start, rows), :]
            errs.append(err_s[j * rows : (j + 1) * rows, :] * weight)
            tm_s[j * rows : (j + 1) * rows, :] = tm_s[j * rows : (j + 1) * rows, :] * weight
        sendt_s[s] = jnp.sum(tm_s[...].T, axis=0, keepdims=True)
        for o in range(n_cplx):
            piece = jnp.zeros_like(errs[0])
            for j in range(slots):
                piece = jnp.where(owners[j] == o, errs[j], piece)
            send_s[s, o] = piece

        @pl.when(s == 0)
        def _():
            pl.semaphore_wait(barrier, plane - 1 + blocks - 1)

        for d in range(1, n_cplx):
            err_copy(s, d).start()
            tm_copy(s, d).start()

        @pl.when(s < parts - 1)
        def _():
            err_copy(s, 0).start()
            tm_copy(s, 0).start()

        @pl.when(s == parts - 1)
        def _():
            recv_s[bz * n_cplx + mine] = send_s[s, mine]
            recvt_s[bz * n_cplx + mine] = sendt_s[s]

        return carry

    lax.fori_loop(0, parts, stage, 0)

    def await_err(zs, count):
        spot = recv_s.at[pl.ds(zs * n_cplx, count)]
        pltpu.make_async_copy(spot, spot, recv_sem.at[zs]).wait()
        spot = recvt_s.at[pl.ds(zs * n_cplx, count)]
        pltpu.make_async_copy(spot, spot, recvt_sem.at[zs]).wait()

    def arrive(d, carry):
        await_err(lax.rem(bz + d, parts), n_cplx)
        return carry

    lax.fori_loop(1, parts, arrive, 0)
    await_err(bz, n_cplx - 1)

    base = 3 * slots
    per_tile = n_cplx * slots

    def pick(at):
        n = jnp.maximum(table_ref[base + at] - 1, 0)
        t = n // per_tile
        o = lax.rem(n, per_tile) // slots
        j = lax.rem(n, slots)
        return t // parts, lax.rem(t, parts) * n_cplx + o, j

    def gather(i, carry):
        yy = i // cells
        cell = lax.rem(i, cells)
        _, src, j = pick(i)
        ysend_s[yy, cell] = recv_s[src]
        line = recvt_s[src]
        short = line[:, 0:rows]
        for q in range(1, slots):
            short = jnp.where(j == q, line[:, q * rows : (q + 1) * rows], short)
        ysendt_s[yy, cell, :, 0:rows] = short
        return carry

    lax.fori_loop(0, blocks * cells, gather, 0)

    def y_copy(d, small):
        to = lax.rem(by + d, blocks)
        src, dst, sem = (
            (ysendt_s, yrecvt_s, yrecvt_sem) if small else (ysend_s, yrecv_s, yrecv_sem)
        )
        return pltpu.make_async_remote_copy(
            src_ref=src.at[to],
            dst_ref=dst.at[by],
            send_sem=ysend_sem.at[int(small), d],
            recv_sem=sem.at[by],
            device_id=(to * parts + bz, mine),
            device_id_type=MESH,
        )

    order = sorted(range(1, blocks), key=lambda d: -min(d, blocks - d))
    for d in order:
        y_copy(d, True).start()
        y_copy(d, False).start()
    yrecv_s[by] = ysend_s[by]
    yrecvt_s[by] = ysendt_s[by]

    def y_wait(ref, sem, ys):
        pltpu.make_async_copy(ref.at[ys], ref.at[ys], sem.at[ys]).wait()

    for d in range(1, blocks):
        y_wait(yrecvt_s, yrecvt_sem, lax.rem(by + d, blocks))

    denoms = []
    best = []
    for m in range(cpx_dev):
        k = mine * cpx_dev + m
        length = lengths_ref[k]
        line = resolved_ref[pl.ds(k, 1), :]
        where = lax.broadcasted_iota(jnp.int32, line.shape, 1)
        total = jnp.sum(
            jnp.where((where < length) & (line > 0), 1.0, 0.0), axis=1, keepdims=True
        )
        own = pltpu.roll(valid(k, length, by), lax.rem(side - bz * rows, side), 1)[:, 0:rows]
        denom = jnp.maximum(own * total, 1.0)
        denoms.append(denom)
        acc = jnp.zeros((1, rows), F32)
        for q in range(blocks):
            at = by * cells + m * blocks + q
            ys, _, _ = pick(at)
            there = table_ref[base + at] > 0
            acc = acc + jnp.where(there, yrecvt_s[ys, m * blocks + q][:, 0:rows], 0.0)
        best.append(jnp.max(acc / denom, axis=1, keepdims=True))
    for m in range(cpx_dev):
        top_s[0, m] = jnp.broadcast_to(best[m], (1, lanes))

    def top_copy(axis, d):
        if axis == 0:
            device, dst, sem, spot = by * parts + lax.rem(bz + d, parts), topz_s, topz_sem, bz
        else:
            device, dst, sem, spot = lax.rem(by + d, blocks) * parts + bz, topy_s, topy_sem, by
        return pltpu.make_async_remote_copy(
            src_ref=top_s.at[axis],
            dst_ref=dst.at[spot],
            send_sem=topsend_sem.at[axis, d],
            recv_sem=sem.at[spot],
            device_id=(device, mine),
            device_id_type=MESH,
        )

    for d in range(1, parts):
        top_copy(0, d).start()

    for d in range(1, blocks):
        y_wait(yrecv_s, yrecv_sem, lax.rem(by + d, blocks))
    for m in range(cpx_dev):
        total = jnp.zeros((rows, side), F32)
        for q in range(blocks):
            at = by * cells + m * blocks + q
            ys, _, _ = pick(at)
            there = table_ref[base + at] > 0
            piece = jnp.where(there, yrecv_s[ys, m * blocks + q], 0.0)
            map_ref[m, :, q * side : (q + 1) * side] = piece
            total = total + piece
        res_ref[pl.ds(m, 1), :] = jnp.sum(total.T, axis=0, keepdims=True) / denoms[m]

    best = top_s[0]
    for d in range(1, parts):
        zs = lax.rem(bz + d, parts)
        y_wait(topz_s, topz_sem, zs)
        best = jnp.maximum(best, topz_s[zs])
    top_s[1] = best
    for d in range(1, blocks):
        top_copy(1, d).start()
    for d in range(1, blocks):
        ys = lax.rem(by + d, blocks)
        y_wait(topy_s, topy_sem, ys)
        best = jnp.maximum(best, topy_s[ys])
    best_ref[...] = best

    def drain(s, count):
        spot = send_s.at[s, pl.ds(0, count)]
        pltpu.make_async_copy(spot, spot, send_sem.at[s]).wait()
        spot = recvt_s.at[pl.ds(0, count)]
        pltpu.make_async_copy(spot, spot, sendt_sem.at[s]).wait()

    def drain_all(s, carry):
        drain(s, n_cplx)
        return carry

    lax.fori_loop(0, parts - 1, drain_all, 0)
    drain(parts - 1, n_cplx - 1)
    for d in range(1, blocks):
        y_copy(d, True).wait_send()
        y_copy(d, False).wait_send()
    for d in range(1, parts):
        top_copy(0, d).wait_send()
    for d in range(1, blocks):
        top_copy(1, d).wait_send()


def shards(pair_tiles, tile_map, lengths, resolved, ln_gain, w_in, w_out, w_head, head_bias):
    n_tile = lax.axis_size("tile")
    n_cplx = lax.axis_size("cplx")
    slots, side, _, chan = pair_tiles.shape
    hid = w_in.shape[1]
    bins = w_head.shape[1]
    complexes, maxres = resolved.shape
    blocks = maxres // side
    cpx_dev = complexes // n_cplx
    rows = maxres // n_tile
    parts = side // rows
    cells = cpx_dev * blocks
    mine = lax.axis_index("cplx")
    device = lax.axis_index("tile") * n_cplx + mine
    own = lax.dynamic_slice_in_dim(tile_map, device * slots, slots).reshape(3 * slots)
    member = tile_map[:, 0] - mine * cpx_dev
    cell = (tile_map[:, 1] * cpx_dev + member) * blocks + tile_map[:, 2]
    cell = jnp.where((tile_map[:, 0] >= 0) & (member >= 0) & (member < cpx_dev), cell, -1)
    number = jnp.arange(tile_map.shape[0], dtype=jnp.int32) + 1
    want = jnp.arange(blocks * cells, dtype=jnp.int32)
    inverse = jnp.sum(jnp.where(cell[None, :] == want[:, None], number[None, :], 0), axis=1)
    table = jnp.concatenate([own, inverse])
    vmem = pl.BlockSpec(memory_space=pltpu.VMEM)
    smem = pl.BlockSpec(memory_space=pltpu.SMEM)
    dma = pltpu.SemaphoreType.DMA
    error_map, residue, best = pl.pallas_call(
        functools.partial(fused_kernel, blocks=blocks, parts=parts, n_cplx=n_cplx),
        in_specs=[smem, smem, pl.BlockSpec(memory_space=pl.ANY)] + [vmem] * 6,
        out_specs=[vmem] * 3,
        out_shape=[
            jax.ShapeDtypeStruct((cpx_dev, rows, maxres), F32),
            jax.ShapeDtypeStruct((cpx_dev, rows), F32),
            jax.ShapeDtypeStruct((cpx_dev, 1, 128), F32),
        ],
        scratch_shapes=[
            pltpu.VMEM((chan + bins, chan), BF16),
            pltpu.VMEM((hid, chan), BF16),
            pltpu.VMEM((bins, hid), BF16),
            pltpu.VMEM((bins, 128), F32),
            pltpu.VMEM((bins, 128), F32),
            pltpu.VMEM((slots, bins, 128), F32),
            pltpu.VMEM((slots, side, side), F32),
            pltpu.VMEM((2, slots * rows, side, chan), BF16),
            pltpu.VMEM((slots * rows, side), F32),
            pltpu.VMEM((128, side), F32),
            pltpu.VMEM((parts, n_cplx, rows, side), F32),
            pltpu.VMEM((parts, 1, 128), F32),
            pltpu.VMEM((parts * n_cplx, rows, side), F32),
            pltpu.VMEM((parts * n_cplx, 1, 128), F32),
            pltpu.VMEM((blocks, cells, rows, side), F32),
            pltpu.VMEM((blocks, cells, 1, 128), F32),
            pltpu.VMEM((blocks, cells, rows, side), F32),
            pltpu.VMEM((blocks, cells, 1, 128), F32),
            pltpu.VMEM((2, cpx_dev, 1, 128), F32),
            pltpu.VMEM((parts, cpx_dev, 1, 128), F32),
            pltpu.VMEM((blocks, cpx_dev, 1, 128), F32),
            dma((2, slots)),
            dma((parts,)),
            dma((parts,)),
            dma((parts,)),
            dma((parts,)),
            dma((2, blocks)),
            dma((blocks,)),
            dma((blocks,)),
            dma((2, max(parts, blocks))),
            dma((parts,)),
            dma((blocks,)),
        ],
        compiler_params=pltpu.CompilerParams(
            collective_id=0, has_side_effects=True, vmem_limit_bytes=60 * 1024 * 1024
        ),
        name="fused",
    )(
        table,
        lengths,
        pair_tiles,
        resolved,
        ln_gain.reshape(1, chan),
        w_in,
        w_out,
        w_head,
        head_bias.reshape(1, bins),
    )
    return error_map, residue, best[:, 0, 0]


def solution(mesh):
    placed = (P(("tile", "cplx"), None, None, None), P(), P(), P(), P(), P(), P(), P(), P())
    return jax.shard_map(
        shards,
        mesh=mesh,
        in_specs=placed,
        out_specs=(P("cplx", "tile", None), P("cplx", "tile"), P("cplx")),
        check_vma=False,
    )
```

```python
import functools
import jax
import jax.numpy as jnp
from jax import lax
from jax.experimental import pallas as pl
from jax.experimental.pallas import tpu as pltpu
from jax.sharding import PartitionSpec as P

EPS = 1e-05
LOG2E = 1.4426950408889634
F32 = jnp.float32
BF16 = jnp.bfloat16
MESH = pl.DeviceIdType.MESH
GROUP = 4
LAG = 2
UNROLL = 4


def fused_kernel(
    tmap_ref,
    lengths_ref,
    x_ref,
    vmap_ref,
    resolved_ref,
    gain_ref,
    w_in_ref,
    w_out_ref,
    w_head_ref,
    bias_ref,
    map_ref,
    res_ref,
    best_ref,
    mix_s,
    w1_s,
    w2_s,
    bias_s,
    cen_s,
    tmw_s,
    weight_s,
    x_s,
    xc_s,
    h_s,
    hd_s,
    rs_s,
    hdc_s,
    rsc_s,
    err_s,
    tm_s,
    tab_v,
    tab_s,
    den_s,
    acc_s,
    sum_s,
    send_s,
    sendt_s,
    recv_s,
    recvt_s,
    yrecv_s,
    yrecvt_s,
    top_s,
    topz_s,
    x_sem,
    tab_sem,
    send_sem,
    sendt_sem,
    recv_sem,
    recvt_sem,
    ysend_sem,
    ysendt_sem,
    yrecv_sem,
    yrecvt_sem,
    topsend_sem,
    topz_sem,
    *,
    blocks,
    parts,
    n_cplx,
):
    slots, side, _, chan = x_ref.shape
    bins = bias_ref.shape[1]
    lanes = 128
    rows = side // parts
    cpx_dev = map_ref.shape[0]
    cells = cpx_dev * blocks
    tile = lax.axis_index("tile")
    mine = lax.axis_index("cplx")
    by = tile // parts
    bz = lax.rem(tile, parts)
    device = tile * n_cplx + mine
    last = parts - 1

    def whole_div(n, d):
        return ((n * (65536 // d + 1)) >> 16) if d > 1 else n

    def x_copy(s, j):
        p = lax.rem(bz + last - s, parts)
        return pltpu.make_async_copy(
            x_ref.at[j, pl.ds(p * rows, rows)],
            x_s.at[pl.ds((s * slots + j) * rows, rows)],
            x_sem.at[s, j],
        )

    def x_start(s, carry):
        for j in range(slots):
            x_copy(s, j).start()
        return carry

    lax.fori_loop(0, parts, x_start, 0)

    barrier = pltpu.get_barrier_semaphore()
    plane = parts * n_cplx

    def greet(d, carry):
        other = lax.rem(bz * n_cplx + mine + d, plane)
        pl.semaphore_signal(
            barrier,
            inc=1,
            device_id=(by * parts + other // n_cplx, lax.rem(other, n_cplx)),
            device_id_type=MESH,
        )
        return carry

    lax.fori_loop(1, plane, greet, 0)
    for d in range(1, blocks):
        pl.semaphore_signal(
            barrier,
            inc=1,
            device_id=(lax.rem(by + d, blocks) * parts + bz, mine),
            device_id_type=MESH,
        )

    r = lax.broadcasted_iota(jnp.int32, (chan, chan), 0)
    c = lax.broadcasted_iota(jnp.int32, (chan, chan), 1)
    mix_s[0:chan, :] = (jnp.where(r == c, 1.0, 0.0) - 1.0 / chan).astype(BF16)
    mix_s[chan : chan + bins, :] = w_head_ref[...]
    w1_s[...] = (w_in_ref[...].astype(F32).T * gain_ref[...]).astype(BF16)
    w2_s[...] = lax.dot_general(
        w_head_ref[...], w_out_ref[...], (((1,), (1,)), ((), ())), preferred_element_type=F32
    ).astype(BF16)
    bias_s[...] = jnp.broadcast_to(bias_ref[...] * LOG2E, (lanes, bins)).T
    b = lax.broadcasted_iota(jnp.int32, (bins, lanes), 0).astype(F32)
    cen_s[...] = (b + 0.5) * (31.0 / (bins - 2))
    pos = lax.broadcasted_iota(jnp.int32, (1, side), 1)

    def stage_a(group, par):
        row = pl.multiple_of(group * GROUP, GROUP)
        x = x_s[pl.ds(row, GROUP), :, :].reshape(GROUP * side, chan)
        first = lax.dot_general(
            mix_s[...], x, (((1,), (1,)), ((), ())), preferred_element_type=F32
        )
        xc = first[:chan]
        var = jnp.mean(xc * xc, axis=0, keepdims=True)
        xc_s[par] = xc.astype(BF16)
        rs_s[par] = lax.rsqrt(var + EPS) * LOG2E
        bias = jnp.concatenate([bias_s[...]] * GROUP, axis=1)
        hd_s[par] = first[chan:] * LOG2E + bias

    def stage_b(par):
        z = jnp.dot(w1_s[...], xc_s[par], preferred_element_type=F32)
        h_s[par] = jnp.maximum(z, 0.0).astype(BF16)
        hdc_s[par] = hd_s[par]
        rsc_s[par] = rs_s[par]

    def stage_c(row, slot, par):
        cen = jnp.concatenate([cen_s[...]] * GROUP, axis=1)
        tmw = jnp.concatenate([tmw_s[slot]] * GROUP, axis=1)
        y = jnp.dot(w2_s[...], h_s[par], preferred_element_type=F32)
        logits = hdc_s[par] + rsc_s[par] * y
        top = jnp.max(logits, axis=0, keepdims=True)
        e = jnp.exp2(logits - top)
        s0 = jnp.sum(e, axis=0, keepdims=True)
        s1 = jnp.sum(e * cen, axis=0, keepdims=True)
        s2 = jnp.sum(e * tmw, axis=0, keepdims=True)
        inv = 1.0 / s0
        expected = s1 * inv
        term = s2 * inv
        for i in range(GROUP):
            err_s[pl.ds(row + i, 1), :] = expected[:, i * side : (i + 1) * side]
            tm_s[pl.ds(row + i, 1), :] = term[:, i * side : (i + 1) * side]

    n = lax.broadcasted_iota(jnp.int32, (1, vmap_ref.shape[1]), 1)
    unit = whole_div(n, slots)
    slot_of = n - unit * slots
    tile_of = whole_div(unit, n_cplx)
    cplx_of = unit - tile_of * n_cplx
    k_all = vmap_ref[0:1, :]
    member = k_all - mine * cpx_dev
    here = (k_all >= 0) & (member >= 0) & (member < cpx_dev)
    key = jnp.where(here, (vmap_ref[1:2, :] * cpx_dev + member) * blocks + vmap_ref[2:3, :], -1)
    near = tile_of - by * parts
    key2 = jnp.where(here & (near >= 0) & (near < parts), near * slots + slot_of, -1)
    want = lax.broadcasted_iota(jnp.int32, (128, n.shape[1]), 0)
    spot = jnp.where(want == key, tile_of * slots + slot_of + 1, 0)
    spot2 = jnp.where(want == key2, cplx_of, 0)
    tab_v[...] = jnp.zeros_like(tab_v)
    for i, wide in enumerate((spot, spot2)):
        folded = jnp.zeros((128, 128), jnp.int32)
        width = wide.shape[1]
        for at in range(0, width, 128):
            piece = wide[:, at : min(at + 128, width)]
            if piece.shape[1] < 128:
                fill = jnp.zeros((128, 128 - piece.shape[1]), jnp.int32)
                piece = jnp.concatenate([piece, fill], axis=1)
            folded = folded + piece
        folded = folded.T
        while folded.shape[0] > 1:
            half = folded.shape[0] // 2
            folded = folded[:half] + folded[half:]
        tab_v[i : i + 1, :] = folded
    tab_copy = pltpu.make_async_copy(tab_v, tab_s, tab_sem.at[0])
    tab_copy.start()

    for j in range(slots):
        x_copy(0, j).wait()
    stage_a(0, 0)
    stage_a(1, 1)
    stage_b(0)
    stage_a(2, 0)

    def valid(k, length, block):
        line = resolved_ref[pl.ds(k, 1), :]
        part = jnp.zeros((1, side), jnp.int32)
        for q in range(blocks):
            part = jnp.where(block == q, line[:, q * side : (q + 1) * side], part)
        return jnp.where((pos + block * side < length) & (part > 0), 1.0, 0.0)

    owners = []
    for j in range(slots):
        at = device * slots + j
        found = tmap_ref[0, at]
        k = jnp.maximum(found, 0)
        length = lengths_ref[k]
        size = jnp.full((bins, lanes), jnp.maximum(length, 19).astype(F32) - 15.0, F32)
        d0 = 1.24 * jnp.exp(jnp.log(size) * (1.0 / 3.0)) - 1.8
        ratio = cen_s[...] / d0
        tmw_s[j] = 1.0 / (1.0 + ratio * ratio)
        row_valid = valid(k, length, jnp.maximum(tmap_ref[1, at], 0))
        col_valid = valid(k, length, jnp.maximum(tmap_ref[2, at], 0))
        col_valid = jnp.where(found >= 0, col_valid, 0.0)
        weight_s[j] = jnp.broadcast_to(row_valid, (side, side)).T * col_valid
        owners.append(jnp.where(found >= 0, whole_div(k, cpx_dev), -1))

    acc_s[...] = jnp.zeros_like(acc_s)
    den_s[...] = jnp.ones_like(den_s)
    for m in range(cpx_dev):
        k = mine * cpx_dev + m
        length = lengths_ref[k]
        line = resolved_ref[pl.ds(k, 1), :]
        where = lax.broadcasted_iota(jnp.int32, line.shape, 1)
        valid_line = jnp.where((where < length) & (line > 0), 1.0, 0.0)
        total = jnp.sum(valid_line, axis=1, keepdims=True)
        for q in range(blocks):
            part = valid_line[:, q * side : (q + 1) * side]
            own = pltpu.roll(part, lax.rem(side - bz * rows, side), 1)
            den_s[q, m : m + 1, :] = jnp.maximum(own * total, 1.0)

    per_stage = slots * rows // GROUP
    per_slot = rows // GROUP
    tm_s[...] = jnp.zeros_like(tm_s)

    def err_copy(s, d):
        p = lax.rem(bz + last - s, parts)
        o = lax.rem(mine + d, n_cplx)
        return pltpu.make_async_remote_copy(
            src_ref=send_s.at[s, o],
            dst_ref=recv_s.at[bz * n_cplx + mine],
            send_sem=send_sem.at[s],
            recv_sem=recv_sem.at[bz],
            device_id=(by * parts + p, o),
            device_id_type=MESH,
        )

    def tm_copy(s, d):
        p = lax.rem(bz + last - s, parts)
        o = lax.rem(mine + d, n_cplx)
        return pltpu.make_async_remote_copy(
            src_ref=sendt_s.at[s],
            dst_ref=recvt_s.at[bz * n_cplx + mine],
            send_sem=sendt_sem.at[s],
            recv_sem=recvt_sem.at[bz],
            device_id=(by * parts + p, o),
            device_id_type=MESH,
        )

    def await_part(zs, count):
        at = recvt_s.at[pl.ds(zs * n_cplx, count)]
        pltpu.make_async_copy(at, at, recvt_sem.at[zs]).wait()
        at = recv_s.at[pl.ds(zs * n_cplx, count)]
        pltpu.make_async_copy(at, at, recv_sem.at[zs]).wait()

    def y_copy(zs, d, small):
        to = lax.rem(by + d, blocks)
        ref, sent, sem = (
            (yrecvt_s, ysendt_sem, yrecvt_sem) if small else (yrecv_s, ysend_sem, yrecv_sem)
        )
        at = pl.ds((by * parts + zs) * slots, slots)
        return pltpu.make_async_remote_copy(
            src_ref=ref.at[at],
            dst_ref=ref.at[at],
            send_sem=sent.at[zs],
            recv_sem=sem.at[by],
            device_id=(to * parts + bz, mine),
            device_id_type=MESH,
        )

    order = sorted(range(1, blocks), key=lambda d: -min(d, blocks - d))

    def forward(s, count):
        zs = lax.rem(bz + s + 1, parts)
        await_part(zs, count)
        from_o = [tab_s[1, zs * slots + j] for j in range(slots)]
        pieces = [jnp.zeros((rows, side), F32)] * slots
        lines = [jnp.zeros((1, rows), F32)] * slots
        for o in range(n_cplx):
            piece = recv_s[zs * n_cplx + o]
            line = recvt_s[zs * n_cplx + o]
            for j in range(slots):
                pieces[j] = jnp.where(from_o[j] == o, piece, pieces[j])
                short = line[:, j * rows : (j + 1) * rows]
                lines[j] = jnp.where(from_o[j] == o, short, lines[j])
        for j in range(slots):
            to = (by * parts + zs) * slots + j
            yrecvt_s[to, :, 0:rows] = lines[j]
            yrecv_s[to] = pieces[j]
        for d in order:
            y_copy(zs, d, True).start()
        for d in order:
            y_copy(zs, d, False).start()

    tab_copy.wait()

    def stage(s, carry):
        @pl.when(s < last)
        def _():
            for j in range(slots):
                x_copy(s + 1, j).wait()

        def body(i, inner):
            g = UNROLL * i
            stop = parts * per_stage - 1
            row = pl.multiple_of(g * GROUP, UNROLL * GROUP)
            for u in range(UNROLL):
                stage_b((u + 1) % 2)
                stage_c(row + u * GROUP, (g + u) // per_slot, u % 2)
                stage_a(jnp.minimum(s * per_stage + g + u + 3, stop), (u + 1) % 2)
            return inner

        lax.fori_loop(0, per_stage // UNROLL, body, 0)

        p = lax.rem(bz + last - s, parts)
        start = pl.multiple_of(p * rows, rows)
        errs = []
        for j in range(slots):
            weight = weight_s[j, pl.ds(start, rows), :]
            errs.append(err_s[j * rows : (j + 1) * rows, :] * weight)
            tm_s[j * rows : (j + 1) * rows, :] = tm_s[j * rows : (j + 1) * rows, :] * weight
        sendt_s[s] = jnp.sum(tm_s[...].T, axis=0, keepdims=True)
        for o in range(n_cplx):
            piece = jnp.zeros_like(errs[0])
            for j in range(slots):
                piece = jnp.where(owners[j] == o, errs[j], piece)
            send_s[s, o] = piece

        @pl.when(s == 0)
        def _():
            pl.semaphore_wait(barrier, plane - 1 + blocks - 1)

        for d in range(1, n_cplx):
            tm_copy(s, d).start()
        for d in range(1, n_cplx):
            err_copy(s, d).start()

        @pl.when(s < last)
        def _():
            tm_copy(s, 0).start()
            err_copy(s, 0).start()

        @pl.when(s == last)
        def _():
            recv_s[bz * n_cplx + mine] = send_s[s, mine]
            recvt_s[bz * n_cplx + mine] = sendt_s[s]

        @pl.when(s >= LAG)
        def _():
            forward(s - LAG, n_cplx)

        return carry

    lax.fori_loop(0, parts, stage, 0)
    for s in range(max(parts - LAG, 0), parts):
        forward(s, n_cplx if s < last else n_cplx - 1)

    def y_wait(ref, sem, ys):
        at = ref.at[pl.ds(ys * parts * slots, parts * slots)]
        pltpu.make_async_copy(at, at, sem.at[ys]).wait()

    for d in range(1, blocks):
        y_wait(yrecvt_s, yrecvt_sem, lax.rem(by + d, blocks))

    for q in range(blocks):
        for m in range(cpx_dev):
            acc = jnp.zeros((1, rows), F32)
            for e in range(blocks):
                found = tab_s[0, (q * cpx_dev + m) * blocks + e]
                line = yrecvt_s[jnp.clip(found - 1, 0, blocks * parts * slots - 1)][:, 0:rows]
                acc = acc + jnp.where(found > 0, line, 0.0)
            acc_s[q, m : m + 1, 0:rows] = acc
    top_s[...] = jnp.max(acc_s[...] / den_s[...], axis=0)

    def top_copy(d):
        return pltpu.make_async_remote_copy(
            src_ref=top_s,
            dst_ref=topz_s.at[bz],
            send_sem=topsend_sem.at[d],
            recv_sem=topz_sem.at[bz],
            device_id=(by * parts + lax.rem(bz + d, parts), mine),
            device_id_type=MESH,
        )

    for d in sorted(range(1, parts), key=lambda d: -min(d, parts - d)):
        top_copy(d).start()

    for d in range(1, blocks):
        y_wait(yrecv_s, yrecv_sem, lax.rem(by + d, blocks))
    for m in range(cpx_dev):
        total = jnp.zeros((rows, side), F32)
        for q in range(blocks):
            found = tab_s[0, (by * cpx_dev + m) * blocks + q]
            piece = jnp.where(found > 0, yrecv_s[jnp.clip(found - 1, 0, blocks * parts * slots - 1)], 0.0)
            map_ref[m, :, q * side : (q + 1) * side] = piece
            total = total + piece
        sum_s[m * rows : (m + 1) * rows, :] = total
    totals = jnp.sum(sum_s[...].T, axis=0, keepdims=True)
    for m in range(cpx_dev):
        denom = den_s[by, m : m + 1, 0:rows]
        res_ref[m : m + 1, :] = totals[:, m * rows : (m + 1) * rows] / denom

    best = top_s[...]
    for d in range(1, parts):
        zs = lax.rem(bz + d, parts)
        pltpu.make_async_copy(topz_s.at[zs], topz_s.at[zs], topz_sem.at[zs]).wait()
        best = jnp.maximum(best, topz_s[zs])
    best = jnp.max(best, axis=1, keepdims=True)
    best_ref[...] = jnp.broadcast_to(best, best_ref.shape)

    def drain(s, count):
        at = send_s.at[s, pl.ds(0, count)]
        pltpu.make_async_copy(at, at, send_sem.at[s]).wait()
        at = recvt_s.at[pl.ds(0, count)]
        pltpu.make_async_copy(at, at, sendt_sem.at[s]).wait()

    def drain_all(s, carry):
        drain(s, n_cplx)
        return carry

    lax.fori_loop(0, last, drain_all, 0)
    drain(last, n_cplx - 1)

    def drain_y(zs, carry):
        at = pl.ds(0, (blocks - 1) * slots)
        pltpu.make_async_copy(yrecvt_s.at[at], yrecvt_s.at[at], ysendt_sem.at[zs]).wait()
        pltpu.make_async_copy(yrecv_s.at[at], yrecv_s.at[at], ysend_sem.at[zs]).wait()
        return carry

    lax.fori_loop(0, parts, drain_y, 0)
    for d in range(1, parts):
        top_copy(d).wait_send()


def shards(pair_tiles, tile_map, lengths, resolved, ln_gain, w_in, w_out, w_head, head_bias):
    n_tile = lax.axis_size("tile")
    n_cplx = lax.axis_size("cplx")
    slots, side, _, chan = pair_tiles.shape
    hid = w_in.shape[1]
    bins = w_head.shape[1]
    complexes, maxres = resolved.shape
    blocks = maxres // side
    cpx_dev = complexes // n_cplx
    rows = maxres // n_tile
    parts = side // rows
    cells = cpx_dev * blocks
    vmem = pl.BlockSpec(memory_space=pltpu.VMEM)
    smem = pl.BlockSpec(memory_space=pltpu.SMEM)
    dma = pltpu.SemaphoreType.DMA
    groups = GROUP * side
    error_map, residue, best = pl.pallas_call(
        functools.partial(fused_kernel, blocks=blocks, parts=parts, n_cplx=n_cplx),
        in_specs=[smem, smem, pl.BlockSpec(memory_space=pl.ANY)] + [vmem] * 7,
        out_specs=[vmem] * 3,
        out_shape=[
            jax.ShapeDtypeStruct((cpx_dev, rows, maxres), F32),
            jax.ShapeDtypeStruct((cpx_dev, rows), F32),
            jax.ShapeDtypeStruct((8, 128), F32),
        ],
        scratch_shapes=[
            pltpu.VMEM((chan + bins, chan), BF16),
            pltpu.VMEM((hid, chan), BF16),
            pltpu.VMEM((bins, hid), BF16),
            pltpu.VMEM((bins, 128), F32),
            pltpu.VMEM((bins, 128), F32),
            pltpu.VMEM((slots, bins, 128), F32),
            pltpu.VMEM((slots, side, side), F32),
            pltpu.VMEM((parts * slots * rows, side, chan), BF16),
            pltpu.VMEM((2, chan, groups), BF16),
            pltpu.VMEM((2, hid, groups), BF16),
            pltpu.VMEM((2, bins, groups), F32),
            pltpu.VMEM((2, 1, groups), F32),
            pltpu.VMEM((2, bins, groups), F32),
            pltpu.VMEM((2, 1, groups), F32),
            pltpu.VMEM((slots * rows, side), F32),
            pltpu.VMEM((128, side), F32),
            pltpu.VMEM((8, 128), jnp.int32),
            pltpu.SMEM((8, 128), jnp.int32),
            pltpu.VMEM((blocks, 8, 128), F32),
            pltpu.VMEM((blocks, 8, 128), F32),
            pltpu.VMEM((128, side), F32),
            pltpu.VMEM((parts, n_cplx, rows, side), F32),
            pltpu.VMEM((parts, 1, 128), F32),
            pltpu.VMEM((parts * n_cplx, rows, side), F32),
            pltpu.VMEM((parts * n_cplx, 1, 128), F32),
            pltpu.VMEM((blocks * parts * slots, rows, side), F32),
            pltpu.VMEM((blocks * parts * slots, 1, 128), F32),
            pltpu.VMEM((8, 128), F32),
            pltpu.VMEM((parts, 8, 128), F32),
            dma((parts, slots)),
            dma((1,)),
            dma((parts,)),
            dma((parts,)),
            dma((parts,)),
            dma((parts,)),
            dma((parts,)),
            dma((parts,)),
            dma((blocks,)),
            dma((blocks,)),
            dma((parts,)),
            dma((parts,)),
        ],
        compiler_params=pltpu.CompilerParams(
            collective_id=0, has_side_effects=True, vmem_limit_bytes=60 * 1024 * 1024
        ),
        name="fused",
    )(
        tile_map.T,
        lengths,
        pair_tiles,
        tile_map.T,
        resolved,
        ln_gain.reshape(1, chan),
        w_in,
        w_out,
        w_head.T,
        head_bias.reshape(1, bins),
    )
    return error_map, residue, best[:cpx_dev, 0]


def solution(mesh):
    placed = (P(("tile", "cplx"), None, None, None), P(), P(), P(), P(), P(), P(), P(), P())
    return jax.shard_map(
        shards,
        mesh=mesh,
        in_specs=placed,
        out_specs=(P("cplx", "tile", None), P("cplx", "tile"), P("cplx")),
        check_vma=False,
    )
```

```python
import functools
import jax
import jax.numpy as jnp
from jax import lax
from jax.experimental import pallas as pl
from jax.experimental.pallas import tpu as pltpu
from jax.sharding import PartitionSpec as P

EPS = 1e-05
LOG2E = 1.4426950408889634
F32 = jnp.float32
BF16 = jnp.bfloat16
MESH = pl.DeviceIdType.MESH
GROUP = 8
LAG = 3
UNROLL = 6


def fused_kernel(
    tmap_ref,
    lengths_ref,
    x_ref,
    vmap_ref,
    resolved_ref,
    gain_ref,
    w_in_ref,
    w_out_ref,
    w_head_ref,
    bias_ref,
    map_ref,
    res_ref,
    best_ref,
    mix_s,
    w1_s,
    w2_s,
    bias_s,
    cen_s,
    tmw_s,
    weight_s,
    x_s,
    xc_s,
    h_s,
    hd_s,
    rs_s,
    hdc_s,
    rsc_s,
    err_s,
    tm_s,
    tab_v,
    tab_s,
    den_s,
    acc_s,
    sum_s,
    send_s,
    sendt_s,
    recv_s,
    recvt_s,
    yrecv_s,
    yrecvt_s,
    top_s,
    topz_s,
    x_sem,
    tab_sem,
    send_sem,
    sendt_sem,
    recv_sem,
    recvt_sem,
    ysend_sem,
    ysendt_sem,
    yrecv_sem,
    yrecvt_sem,
    topsend_sem,
    topz_sem,
    *,
    blocks,
    parts,
    n_cplx,
):
    slots, side, _, chan = x_ref.shape
    bins = bias_ref.shape[1]
    lanes = 128
    rows = side // parts
    cpx_dev = map_ref.shape[0]
    cells = cpx_dev * blocks
    tile = lax.axis_index("tile")
    mine = lax.axis_index("cplx")
    by = tile // parts
    bz = lax.rem(tile, parts)
    device = tile * n_cplx + mine
    last = parts - 1

    def whole_div(n, d):
        return ((n * (65536 // d + 1)) >> 16) if d > 1 else n

    def offset(s):
        return parts // 2 + (1 - 2 * (s & 1)) * ((s + 1) >> 1)

    def x_copy(s, j):
        p = lax.rem(bz + offset(s), parts)
        return pltpu.make_async_copy(
            x_ref.at[j, pl.ds(p * rows, rows)],
            x_s.at[pl.ds((s * slots + j) * rows, rows)],
            x_sem.at[s, j],
        )

    def x_start(s, carry):
        for j in range(slots):
            x_copy(s, j).start()
        return carry

    lax.fori_loop(0, parts, x_start, 0)

    barrier = pltpu.get_barrier_semaphore()
    plane = parts * n_cplx

    for dz in range(parts):
        to = by * parts + lax.rem(bz + dz, parts)
        for d in range(1 if dz == 0 else 0, n_cplx):
            pl.semaphore_signal(
                barrier,
                inc=1,
                device_id=(to, lax.rem(mine + d, n_cplx)),
                device_id_type=MESH,
            )
    for d in range(1, blocks):
        pl.semaphore_signal(
            barrier,
            inc=1,
            device_id=(lax.rem(by + d, blocks) * parts + bz, mine),
            device_id_type=MESH,
        )

    r = lax.broadcasted_iota(jnp.int32, (chan, chan), 0)
    c = lax.broadcasted_iota(jnp.int32, (chan, chan), 1)
    mix_s[0:chan, :] = (jnp.where(r == c, 1.0, 0.0) - 1.0 / chan).astype(BF16)
    mix_s[chan : chan + bins, :] = w_head_ref[...]
    w1_s[...] = (w_in_ref[...].astype(F32).T * gain_ref[...]).astype(BF16)
    w2_s[...] = lax.dot_general(
        w_head_ref[...], w_out_ref[...], (((1,), (1,)), ((), ())), preferred_element_type=F32
    ).astype(BF16)
    bias_s[...] = jnp.broadcast_to(bias_ref[...] * LOG2E, (lanes, bins)).T
    b = lax.broadcasted_iota(jnp.int32, (bins, lanes), 0).astype(F32)
    cen_s[...] = (b + 0.5) * (31.0 / (bins - 2))
    pos = lax.broadcasted_iota(jnp.int32, (1, side), 1)

    def stage_a(group, par):
        row = pl.multiple_of(group * GROUP, GROUP)
        x = x_s[pl.ds(row, GROUP), :, :].reshape(GROUP * side, chan)
        first = lax.dot_general(
            mix_s[...], x, (((1,), (1,)), ((), ())), preferred_element_type=F32
        )
        xc = first[:chan]
        var = jnp.mean(xc * xc, axis=0, keepdims=True)
        xc_s[par] = xc.astype(BF16)
        rs_s[par] = lax.rsqrt(var + EPS) * LOG2E
        bias = jnp.concatenate([bias_s[...]] * GROUP, axis=1)
        hd_s[par] = first[chan:] * LOG2E + bias

    def stage_b(par):
        z = jnp.dot(w1_s[...], xc_s[par], preferred_element_type=F32)
        h_s[par] = jnp.maximum(z, 0.0).astype(BF16)
        hdc_s[par] = hd_s[par]
        rsc_s[par] = rs_s[par]

    def stage_c(row, slot, par):
        cen = jnp.concatenate([cen_s[...]] * GROUP, axis=1)
        tmw = jnp.concatenate([tmw_s[slot]] * GROUP, axis=1)
        y = jnp.dot(w2_s[...], h_s[par], preferred_element_type=F32)
        logits = hdc_s[par] + rsc_s[par] * y
        top = jnp.max(logits, axis=0, keepdims=True)
        e = jnp.exp2(logits - top)
        s0 = jnp.sum(e, axis=0, keepdims=True)
        s1 = jnp.sum(e * cen, axis=0, keepdims=True)
        s2 = jnp.sum(e * tmw, axis=0, keepdims=True)
        inv = 1.0 / s0
        expected = s1 * inv
        term = s2 * inv
        for i in range(GROUP):
            err_s[pl.ds(row + i, 1), :] = expected[:, i * side : (i + 1) * side]
            tm_s[pl.ds(row + i, 1), :] = term[:, i * side : (i + 1) * side]

    n = lax.broadcasted_iota(jnp.int32, (1, vmap_ref.shape[1]), 1)
    unit = whole_div(n, slots)
    slot_of = n - unit * slots
    tile_of = whole_div(unit, n_cplx)
    cplx_of = unit - tile_of * n_cplx
    k_all = vmap_ref[0:1, :]
    member = k_all - mine * cpx_dev
    here = (k_all >= 0) & (member >= 0) & (member < cpx_dev)
    key = jnp.where(here, (vmap_ref[1:2, :] * cpx_dev + member) * blocks + vmap_ref[2:3, :], -1)
    near = tile_of - by * parts
    key2 = jnp.where(here & (near >= 0) & (near < parts), near * slots + slot_of, -1)
    want = lax.broadcasted_iota(jnp.int32, (128, n.shape[1]), 0)
    spot = jnp.where(want == key, tile_of * slots + slot_of + 1, 0)
    spot2 = jnp.where(want == key2, cplx_of, 0)
    tab_v[...] = jnp.zeros_like(tab_v)
    for i, wide in enumerate((spot, spot2)):
        folded = jnp.zeros((128, 128), jnp.int32)
        width = wide.shape[1]
        for at in range(0, width, 128):
            piece = wide[:, at : min(at + 128, width)]
            if piece.shape[1] < 128:
                fill = jnp.zeros((128, 128 - piece.shape[1]), jnp.int32)
                piece = jnp.concatenate([piece, fill], axis=1)
            folded = folded + piece
        folded = folded.T
        while folded.shape[0] > 1:
            half = folded.shape[0] // 2
            folded = folded[:half] + folded[half:]
        tab_v[i : i + 1, :] = folded
    tab_copy = pltpu.make_async_copy(tab_v, tab_s, tab_sem.at[0])
    tab_copy.start()

    for j in range(slots):
        x_copy(0, j).wait()
    stage_a(0, 0)
    stage_a(1, 1)
    stage_b(0)
    stage_a(2, 0)

    def valid(k, length, block):
        line = resolved_ref[pl.ds(k, 1), :]
        part = jnp.zeros((1, side), jnp.int32)
        for q in range(blocks):
            part = jnp.where(block == q, line[:, q * side : (q + 1) * side], part)
        return jnp.where((pos + block * side < length) & (part > 0), 1.0, 0.0)

    owners = []
    for j in range(slots):
        at = device * slots + j
        found = tmap_ref[0, at]
        k = jnp.maximum(found, 0)
        length = lengths_ref[k]
        size = jnp.full((bins, lanes), jnp.maximum(length, 19).astype(F32) - 15.0, F32)
        d0 = 1.24 * jnp.exp(jnp.log(size) * (1.0 / 3.0)) - 1.8
        ratio = cen_s[...] / d0
        tmw_s[j] = 1.0 / (1.0 + ratio * ratio)
        row_valid = valid(k, length, jnp.maximum(tmap_ref[1, at], 0))
        col_valid = valid(k, length, jnp.maximum(tmap_ref[2, at], 0))
        col_valid = jnp.where(found >= 0, col_valid, 0.0)
        weight_s[j] = jnp.broadcast_to(row_valid, (side, side)).T * col_valid
        owners.append(jnp.where(found >= 0, whole_div(k, cpx_dev), -1))

    acc_s[...] = jnp.zeros_like(acc_s)
    den_s[...] = jnp.ones_like(den_s)
    for m in range(cpx_dev):
        k = mine * cpx_dev + m
        length = lengths_ref[k]
        line = resolved_ref[pl.ds(k, 1), :]
        where = lax.broadcasted_iota(jnp.int32, line.shape, 1)
        valid_line = jnp.where((where < length) & (line > 0), 1.0, 0.0)
        total = jnp.sum(valid_line, axis=1, keepdims=True)
        for q in range(blocks):
            part = valid_line[:, q * side : (q + 1) * side]
            own = pltpu.roll(part, lax.rem(side - bz * rows, side), 1)
            den_s[q, m : m + 1, :] = jnp.maximum(own * total, 1.0)

    per_stage = slots * rows // GROUP
    per_slot = rows // GROUP
    tm_s[...] = jnp.zeros_like(tm_s)

    def err_copy(s, d):
        p = lax.rem(bz + offset(s), parts)
        o = lax.rem(mine + d, n_cplx)
        return pltpu.make_async_remote_copy(
            src_ref=send_s.at[s, o],
            dst_ref=recv_s.at[bz * n_cplx + mine],
            send_sem=send_sem.at[s],
            recv_sem=recv_sem.at[bz],
            device_id=(by * parts + p, o),
            device_id_type=MESH,
        )

    def tm_copy(s, d):
        p = lax.rem(bz + offset(s), parts)
        o = lax.rem(mine + d, n_cplx)
        return pltpu.make_async_remote_copy(
            src_ref=sendt_s.at[s],
            dst_ref=recvt_s.at[bz * n_cplx + mine],
            send_sem=sendt_sem.at[s],
            recv_sem=recvt_sem.at[bz],
            device_id=(by * parts + p, o),
            device_id_type=MESH,
        )

    def await_part(zs, count):
        at = recvt_s.at[pl.ds(zs * n_cplx, count)]
        pltpu.make_async_copy(at, at, recvt_sem.at[zs]).wait()
        at = recv_s.at[pl.ds(zs * n_cplx, count)]
        pltpu.make_async_copy(at, at, recv_sem.at[zs]).wait()

    def y_copy(zs, d, small):
        to = lax.rem(by + d, blocks)
        ref, sent, sem = (
            (yrecvt_s, ysendt_sem, yrecvt_sem) if small else (yrecv_s, ysend_sem, yrecv_sem)
        )
        at = pl.ds((by * parts + zs) * slots, slots)
        return pltpu.make_async_remote_copy(
            src_ref=ref.at[at],
            dst_ref=ref.at[at],
            send_sem=sent.at[zs],
            recv_sem=sem.at[by],
            device_id=(to * parts + bz, mine),
            device_id_type=MESH,
        )

    order = sorted(range(1, blocks), key=lambda d: -min(d, blocks - d))

    def forward(s, count):
        zs = lax.rem(bz + parts - offset(s), parts)
        await_part(zs, count)
        from_o = [tab_s[1, zs * slots + j] for j in range(slots)]
        pieces = [jnp.zeros((rows, side), F32)] * slots
        lines = [jnp.zeros((1, rows), F32)] * slots
        for o in range(n_cplx):
            piece = recv_s[zs * n_cplx + o]
            line = recvt_s[zs * n_cplx + o]
            for j in range(slots):
                pieces[j] = jnp.where(from_o[j] == o, piece, pieces[j])
                short = line[:, j * rows : (j + 1) * rows]
                lines[j] = jnp.where(from_o[j] == o, short, lines[j])
        for j in range(slots):
            to = (by * parts + zs) * slots + j
            yrecvt_s[to, :, 0:rows] = lines[j]
            yrecv_s[to] = pieces[j]
        for d in order:
            y_copy(zs, d, True).start()
        for d in order:
            y_copy(zs, d, False).start()

    tab_copy.wait()

    def stage(s, carry):
        @pl.when(s < last)
        def _():
            for j in range(slots):
                x_copy(s + 1, j).wait()

        def body(i, inner):
            g = UNROLL * i
            stop = parts * per_stage - 1
            row = pl.multiple_of(g * GROUP, UNROLL * GROUP)
            for u in range(UNROLL):
                stage_b((u + 1) % 2)
                stage_c(row + u * GROUP, (g + u) // per_slot, u % 2)
                stage_a(jnp.minimum(s * per_stage + g + u + 3, stop), (u + 1) % 2)
            return inner

        lax.fori_loop(0, per_stage // UNROLL, body, 0)

        p = lax.rem(bz + offset(s), parts)
        start = pl.multiple_of(p * rows, rows)
        errs = []
        for j in range(slots):
            weight = weight_s[j, pl.ds(start, rows), :]
            errs.append(err_s[j * rows : (j + 1) * rows, :] * weight)
            tm_s[j * rows : (j + 1) * rows, :] = tm_s[j * rows : (j + 1) * rows, :] * weight
        sendt_s[s] = jnp.sum(tm_s[...].T, axis=0, keepdims=True)
        for o in range(n_cplx):
            piece = jnp.zeros_like(errs[0])
            for j in range(slots):
                piece = jnp.where(owners[j] == o, errs[j], piece)
            send_s[s, o] = piece

        @pl.when(s == 0)
        def _():
            pl.semaphore_wait(barrier, plane - 1 + blocks - 1)

        for d in range(1, n_cplx):
            tm_copy(s, d).start()
        for d in range(1, n_cplx):
            err_copy(s, d).start()

        @pl.when(s < last)
        def _():
            tm_copy(s, 0).start()
            err_copy(s, 0).start()

        @pl.when(s == last)
        def _():
            recv_s[bz * n_cplx + mine] = send_s[s, mine]
            recvt_s[bz * n_cplx + mine] = sendt_s[s]

        @pl.when(s >= LAG)
        def _():
            forward(s - LAG, n_cplx)

        return carry

    lax.fori_loop(0, parts, stage, 0)
    for s in range(max(parts - LAG, 0), parts):
        forward(s, n_cplx if s < last else n_cplx - 1)

    def y_wait(ref, sem, ys):
        at = ref.at[pl.ds(ys * parts * slots, parts * slots)]
        pltpu.make_async_copy(at, at, sem.at[ys]).wait()

    for d in range(1, blocks):
        y_wait(yrecvt_s, yrecvt_sem, lax.rem(by + d, blocks))

    for q in range(blocks):
        for m in range(cpx_dev):
            acc = jnp.zeros((1, rows), F32)
            for e in range(blocks):
                found = tab_s[0, (q * cpx_dev + m) * blocks + e]
                line = yrecvt_s[jnp.clip(found - 1, 0, blocks * parts * slots - 1)][:, 0:rows]
                acc = acc + jnp.where(found > 0, line, 0.0)
            acc_s[q, m : m + 1, 0:rows] = acc
    top_s[...] = jnp.max(acc_s[...] / den_s[...], axis=0)

    def top_copy(d):
        return pltpu.make_async_remote_copy(
            src_ref=top_s,
            dst_ref=topz_s.at[bz],
            send_sem=topsend_sem.at[d],
            recv_sem=topz_sem.at[bz],
            device_id=(by * parts + lax.rem(bz + d, parts), mine),
            device_id_type=MESH,
        )

    for d in sorted(range(1, parts), key=lambda d: -min(d, parts - d)):
        top_copy(d).start()

    for d in range(1, blocks):
        y_wait(yrecv_s, yrecv_sem, lax.rem(by + d, blocks))
    for m in range(cpx_dev):
        total = jnp.zeros((rows, side), F32)
        for q in range(blocks):
            found = tab_s[0, (by * cpx_dev + m) * blocks + q]
            piece = jnp.where(found > 0, yrecv_s[jnp.clip(found - 1, 0, blocks * parts * slots - 1)], 0.0)
            map_ref[m, :, q * side : (q + 1) * side] = piece
            total = total + piece
        sum_s[m * rows : (m + 1) * rows, :] = total
    totals = jnp.sum(sum_s[...].T, axis=0, keepdims=True)
    for m in range(cpx_dev):
        denom = den_s[by, m : m + 1, 0:rows]
        res_ref[m : m + 1, :] = totals[:, m * rows : (m + 1) * rows] / denom

    best = top_s[...]
    for d in range(1, parts):
        zs = lax.rem(bz + d, parts)
        pltpu.make_async_copy(topz_s.at[zs], topz_s.at[zs], topz_sem.at[zs]).wait()
        best = jnp.maximum(best, topz_s[zs])
    best = jnp.broadcast_to(jnp.max(best, axis=1, keepdims=True), (8, lanes))
    down = lax.broadcasted_iota(jnp.int32, (8, lanes), 0)
    across = lax.broadcasted_iota(jnp.int32, (8, lanes), 1)
    best_ref[...] = jnp.sum(jnp.where(down == across, best, 0.0), axis=0, keepdims=True)

    def drain(s, count):
        at = send_s.at[s, pl.ds(0, count)]
        pltpu.make_async_copy(at, at, send_sem.at[s]).wait()
        at = recvt_s.at[pl.ds(0, count)]
        pltpu.make_async_copy(at, at, sendt_sem.at[s]).wait()

    def drain_all(s, carry):
        drain(s, n_cplx)
        return carry

    lax.fori_loop(0, last, drain_all, 0)
    drain(last, n_cplx - 1)

    def drain_y(zs, carry):
        at = pl.ds(0, (blocks - 1) * slots)
        pltpu.make_async_copy(yrecvt_s.at[at], yrecvt_s.at[at], ysendt_sem.at[zs]).wait()
        pltpu.make_async_copy(yrecv_s.at[at], yrecv_s.at[at], ysend_sem.at[zs]).wait()
        return carry

    lax.fori_loop(0, parts, drain_y, 0)
    for d in range(1, parts):
        top_copy(d).wait_send()


def hand_out(map_in, res_in, best_in, map_ref, res_ref, best_ref):
    map_ref[...] = map_in[...]
    res_ref[...] = res_in[...]
    best_ref[...] = best_in[:, 0 : best_ref.shape[1]]


def shards(pair_tiles, tile_map, lengths, resolved, ln_gain, w_in, w_out, w_head, head_bias):
    n_tile = lax.axis_size("tile")
    n_cplx = lax.axis_size("cplx")
    slots, side, _, chan = pair_tiles.shape
    hid = w_in.shape[1]
    bins = w_head.shape[1]
    complexes, maxres = resolved.shape
    blocks = maxres // side
    cpx_dev = complexes // n_cplx
    rows = maxres // n_tile
    parts = side // rows
    cells = cpx_dev * blocks
    vmem = pl.BlockSpec(memory_space=pltpu.VMEM)
    smem = pl.BlockSpec(memory_space=pltpu.SMEM)
    dma = pltpu.SemaphoreType.DMA
    groups = GROUP * side
    error_map, residue, best = pl.pallas_call(
        functools.partial(fused_kernel, blocks=blocks, parts=parts, n_cplx=n_cplx),
        in_specs=[smem, smem, pl.BlockSpec(memory_space=pl.ANY)] + [vmem] * 7,
        out_specs=[vmem] * 3,
        out_shape=[
            jax.ShapeDtypeStruct((cpx_dev, rows, maxres), F32),
            jax.ShapeDtypeStruct((cpx_dev, rows), F32),
            jax.ShapeDtypeStruct((1, 128), F32),
        ],
        scratch_shapes=[
            pltpu.VMEM((chan + bins, chan), BF16),
            pltpu.VMEM((hid, chan), BF16),
            pltpu.VMEM((bins, hid), BF16),
            pltpu.VMEM((bins, 128), F32),
            pltpu.VMEM((bins, 128), F32),
            pltpu.VMEM((slots, bins, 128), F32),
            pltpu.VMEM((slots, side, side), F32),
            pltpu.VMEM((parts * slots * rows, side, chan), BF16),
            pltpu.VMEM((2, chan, groups), BF16),
            pltpu.VMEM((2, hid, groups), BF16),
            pltpu.VMEM((2, bins, groups), F32),
            pltpu.VMEM((2, 1, groups), F32),
            pltpu.VMEM((2, bins, groups), F32),
            pltpu.VMEM((2, 1, groups), F32),
            pltpu.VMEM((slots * rows, side), F32),
            pltpu.VMEM((128, side), F32),
            pltpu.VMEM((8, 128), jnp.int32),
            pltpu.SMEM((8, 128), jnp.int32),
            pltpu.VMEM((blocks, 8, 128), F32),
            pltpu.VMEM((blocks, 8, 128), F32),
            pltpu.VMEM((128, side), F32),
            pltpu.VMEM((parts, n_cplx, rows, side), F32),
            pltpu.VMEM((parts, 1, 128), F32),
            pltpu.VMEM((parts * n_cplx, rows, side), F32),
            pltpu.VMEM((parts * n_cplx, 1, 128), F32),
            pltpu.VMEM((blocks * parts * slots, rows, side), F32),
            pltpu.VMEM((blocks * parts * slots, 1, 128), F32),
            pltpu.VMEM((8, 128), F32),
            pltpu.VMEM((parts, 8, 128), F32),
            dma((parts, slots)),
            dma((1,)),
            dma((parts,)),
            dma((parts,)),
            dma((parts,)),
            dma((parts,)),
            dma((parts,)),
            dma((parts,)),
            dma((blocks,)),
            dma((blocks,)),
            dma((parts,)),
            dma((parts,)),
        ],
        compiler_params=pltpu.CompilerParams(
            collective_id=0, has_side_effects=True, vmem_limit_bytes=60 * 1024 * 1024
        ),
        name="fused",
    )(
        tile_map.T,
        lengths,
        pair_tiles,
        tile_map.T,
        resolved,
        ln_gain.reshape(1, chan),
        w_in,
        w_out,
        w_head.T,
        head_bias.reshape(1, bins),
    )
    error_map, residue, best = pl.pallas_call(
        hand_out,
        in_specs=[vmem] * 3,
        out_specs=[vmem] * 3,
        out_shape=[
            jax.ShapeDtypeStruct(error_map.shape, F32),
            jax.ShapeDtypeStruct(residue.shape, F32),
            jax.ShapeDtypeStruct((1, cpx_dev), F32),
        ],
        name="hand_out",
    )(error_map, residue, best)
    return error_map, residue, best.reshape(cpx_dev)


def solution(mesh):
    placed = (P(("tile", "cplx"), None, None, None), P(), P(), P(), P(), P(), P(), P(), P())
    return jax.shard_map(
        shards,
        mesh=mesh,
        in_specs=placed,
        out_specs=(P("cplx", "tile", None), P("cplx", "tile"), P("cplx")),
        check_vma=False,
    )
```

```python
import functools
import jax
import jax.numpy as jnp
from jax import lax
from jax.experimental import pallas as pl
from jax.experimental.pallas import tpu as pltpu
from jax.sharding import PartitionSpec as P

EPS = 1e-05
LOG2E = 1.4426950408889634
F32 = jnp.float32
BF16 = jnp.bfloat16
MESH = pl.DeviceIdType.MESH
GROUP = 8
LAG = 3
UNROLL = 6


def fused_kernel(
    tmap_h,
    lengths_h,
    x_ref,
    resolved_h,
    gain_h,
    w_in_h,
    w_out_h,
    w_head_h,
    bias_h,
    map_ref,
    res_ref,
    best_ref,
    tmap_ref,
    lengths_ref,
    vmap_ref,
    resolved_ref,
    gain_ref,
    w_in_ref,
    w_out_ref,
    w_head_ref,
    bias_ref,
    in_sem,
    mix_s,
    w1_s,
    w2_s,
    bias_s,
    cen_s,
    tmw_s,
    weight_s,
    x_s,
    xc_s,
    h_s,
    hd_s,
    rs_s,
    err_s,
    tm_s,
    tab_v,
    tab_s,
    den_s,
    acc_s,
    sum_s,
    send_s,
    sendt_s,
    recv_s,
    recvt_s,
    yrecv_s,
    yrecvt_s,
    top_s,
    topz_s,
    x_sem,
    tab_sem,
    send_sem,
    sendt_sem,
    recv_sem,
    recvt_sem,
    ysend_sem,
    ysendt_sem,
    yrecv_sem,
    yrecvt_sem,
    topsend_sem,
    topz_sem,
    *,
    blocks,
    parts,
    n_cplx,
):
    slots, side, _, chan = x_ref.shape
    bins = bias_h.shape[1]
    lanes = 128
    rows = side // parts
    cpx_dev = map_ref.shape[0]
    cells = cpx_dev * blocks
    tile = lax.axis_index("tile")
    mine = lax.axis_index("cplx")
    by = tile // parts
    bz = lax.rem(tile, parts)
    device = tile * n_cplx + mine
    last = parts - 1

    def whole_div(n, d):
        return ((n * (65536 // d + 1)) >> 16) if d > 1 else n

    def offset(s):
        return parts // 2 + (1 - 2 * (s & 1)) * ((s + 1) >> 1)

    def x_copy(s, j):
        p = lax.rem(bz + offset(s), parts)
        return pltpu.make_async_copy(
            x_ref.at[j, pl.ds(p * rows, rows)],
            x_s.at[pl.ds((s * slots + j) * rows, rows)],
            x_sem.at[s, j],
        )

    def x_start(s, carry):
        for j in range(slots):
            x_copy(s, j).start()
        return carry

    def bring(i):
        pairs = (
            (w_head_h, w_head_ref),
            (bias_h, bias_ref),
            (w_in_h, w_in_ref),
            (gain_h, gain_ref),
            (w_out_h, w_out_ref),
            (tmap_h, vmap_ref),
            (tmap_h, tmap_ref),
            (lengths_h, lengths_ref),
            (resolved_h, resolved_ref),
        )
        return pltpu.make_async_copy(*pairs[i], in_sem.at[i])

    bring(0).start()
    for j in range(slots):
        x_copy(0, j).start()
    for i in range(1, 9):
        bring(i).start()
    lax.fori_loop(1, parts, x_start, 0)

    barrier = pltpu.get_barrier_semaphore()
    plane = parts * n_cplx

    for dz in range(parts):
        to = by * parts + lax.rem(bz + dz, parts)
        for d in range(1 if dz == 0 else 0, n_cplx):
            pl.semaphore_signal(
                barrier,
                inc=1,
                device_id=(to, lax.rem(mine + d, n_cplx)),
                device_id_type=MESH,
            )
    for d in range(1, blocks):
        pl.semaphore_signal(
            barrier,
            inc=1,
            device_id=(lax.rem(by + d, blocks) * parts + bz, mine),
            device_id_type=MESH,
        )

    for i in range(9):
        bring(i).wait()
    r = lax.broadcasted_iota(jnp.int32, (chan, chan), 0)
    c = lax.broadcasted_iota(jnp.int32, (chan, chan), 1)
    mix_s[0:chan, :] = (jnp.where(r == c, 1.0, 0.0) - 1.0 / chan).astype(BF16)
    mix_s[chan : chan + bins, :] = w_head_ref[...]
    w1_s[...] = (w_in_ref[...].astype(F32).T * gain_ref[...]).astype(BF16)
    w2_s[...] = lax.dot_general(
        w_head_ref[...], w_out_ref[...], (((1,), (1,)), ((), ())), preferred_element_type=F32
    ).astype(BF16)
    bias_s[...] = jnp.broadcast_to(bias_ref[...] * LOG2E, (lanes, bins)).T
    b = lax.broadcasted_iota(jnp.int32, (bins, lanes), 0).astype(F32)
    cen_s[...] = (b + 0.5) * (31.0 / (bins - 2))
    pos = lax.broadcasted_iota(jnp.int32, (1, side), 1)

    def stage_a(group, par, keep):
        row = pl.multiple_of(group * GROUP, GROUP)
        x = x_s[pl.ds(row, GROUP), :, :].reshape(GROUP * side, chan)
        first = lax.dot_general(
            mix_s[...], x, (((1,), (1,)), ((), ())), preferred_element_type=F32
        )
        xc = first[:chan]
        var = jnp.mean(xc * xc, axis=0, keepdims=True)
        xc_s[par] = xc.astype(BF16)
        rs_s[keep] = lax.rsqrt(var + EPS) * LOG2E
        bias = jnp.concatenate([bias_s[...]] * GROUP, axis=1)
        hd_s[keep] = first[chan:] * LOG2E + bias

    def stage_b(par):
        z = jnp.dot(w1_s[...], xc_s[par], preferred_element_type=F32)
        h_s[par] = jnp.maximum(z, 0.0).astype(BF16)

    def stage_c(row, slot, par, keep):
        cen = jnp.concatenate([cen_s[...]] * GROUP, axis=1)
        tmw = jnp.concatenate([tmw_s[slot]] * GROUP, axis=1)
        y = jnp.dot(w2_s[...], h_s[par], preferred_element_type=F32)
        logits = hd_s[keep] + rs_s[keep] * y
        top = jnp.max(logits, axis=0, keepdims=True)
        e = jnp.exp2(logits - top)
        s0 = jnp.sum(e, axis=0, keepdims=True)
        s1 = jnp.sum(e * cen, axis=0, keepdims=True)
        s2 = jnp.sum(e * tmw, axis=0, keepdims=True)
        inv = 1.0 / s0
        expected = s1 * inv
        term = s2 * inv
        for i in range(GROUP):
            err_s[pl.ds(row + i, 1), :] = expected[:, i * side : (i + 1) * side]
            tm_s[pl.ds(row + i, 1), :] = term[:, i * side : (i + 1) * side]

    n = lax.broadcasted_iota(jnp.int32, (1, vmap_ref.shape[1]), 1)
    unit = whole_div(n, slots)
    slot_of = n - unit * slots
    tile_of = whole_div(unit, n_cplx)
    cplx_of = unit - tile_of * n_cplx
    k_all = vmap_ref[0:1, :]
    member = k_all - mine * cpx_dev
    here = (k_all >= 0) & (member >= 0) & (member < cpx_dev)
    key = jnp.where(here, (vmap_ref[1:2, :] * cpx_dev + member) * blocks + vmap_ref[2:3, :], -1)
    near = tile_of - by * parts
    key2 = jnp.where(here & (near >= 0) & (near < parts), near * slots + slot_of, -1)
    want = lax.broadcasted_iota(jnp.int32, (128, n.shape[1]), 0)
    spot = jnp.where(want == key, tile_of * slots + slot_of + 1, 0)
    spot2 = jnp.where(want == key2, cplx_of, 0)
    tab_v[...] = jnp.zeros_like(tab_v)
    for i, wide in enumerate((spot, spot2)):
        folded = jnp.zeros((128, 128), jnp.int32)
        width = wide.shape[1]
        for at in range(0, width, 128):
            piece = wide[:, at : min(at + 128, width)]
            if piece.shape[1] < 128:
                fill = jnp.zeros((128, 128 - piece.shape[1]), jnp.int32)
                piece = jnp.concatenate([piece, fill], axis=1)
            folded = folded + piece
        folded = folded.T
        while folded.shape[0] > 1:
            half = folded.shape[0] // 2
            folded = folded[:half] + folded[half:]
        tab_v[i : i + 1, :] = folded
    tab_copy = pltpu.make_async_copy(tab_v, tab_s, tab_sem.at[0])
    tab_copy.start()

    x_copy(0, 0).wait()
    stage_a(0, 0, 0)
    stage_a(1, 1, 1)
    for j in range(1, slots):
        x_copy(0, j).wait()
    stage_b(0)
    stage_a(2, 0, 2)

    def valid(k, length, block):
        line = resolved_ref[pl.ds(k, 1), :]
        part = jnp.zeros((1, side), jnp.int32)
        for q in range(blocks):
            part = jnp.where(block == q, line[:, q * side : (q + 1) * side], part)
        return jnp.where((pos + block * side < length) & (part > 0), 1.0, 0.0)

    owners = []
    for j in range(slots):
        at = device * slots + j
        found = tmap_ref[0, at]
        k = jnp.maximum(found, 0)
        length = lengths_ref[k]
        size = jnp.full((bins, lanes), jnp.maximum(length, 19).astype(F32) - 15.0, F32)
        d0 = 1.24 * jnp.exp(jnp.log(size) * (1.0 / 3.0)) - 1.8
        ratio = cen_s[...] / d0
        tmw_s[j] = 1.0 / (1.0 + ratio * ratio)
        row_valid = valid(k, length, jnp.maximum(tmap_ref[1, at], 0))
        col_valid = valid(k, length, jnp.maximum(tmap_ref[2, at], 0))
        col_valid = jnp.where(found >= 0, col_valid, 0.0)
        weight_s[j] = jnp.broadcast_to(row_valid, (side, side)).T * col_valid
        owners.append(jnp.where(found >= 0, whole_div(k, cpx_dev), -1))

    acc_s[...] = jnp.zeros_like(acc_s)
    den_s[...] = jnp.ones_like(den_s)
    for m in range(cpx_dev):
        k = mine * cpx_dev + m
        length = lengths_ref[k]
        line = resolved_ref[pl.ds(k, 1), :]
        where = lax.broadcasted_iota(jnp.int32, line.shape, 1)
        valid_line = jnp.where((where < length) & (line > 0), 1.0, 0.0)
        total = jnp.sum(valid_line, axis=1, keepdims=True)
        for q in range(blocks):
            part = valid_line[:, q * side : (q + 1) * side]
            own = pltpu.roll(part, lax.rem(side - bz * rows, side), 1)
            den_s[q, m : m + 1, :] = jnp.maximum(own * total, 1.0)

    per_stage = slots * rows // GROUP
    per_slot = rows // GROUP
    tm_s[...] = jnp.zeros_like(tm_s)

    def err_copy(s, d):
        p = lax.rem(bz + offset(s), parts)
        o = lax.rem(mine + d, n_cplx)
        return pltpu.make_async_remote_copy(
            src_ref=send_s.at[s, o],
            dst_ref=recv_s.at[bz * n_cplx + mine],
            send_sem=send_sem.at[s],
            recv_sem=recv_sem.at[bz],
            device_id=(by * parts + p, o),
            device_id_type=MESH,
        )

    def tm_copy(s, d):
        p = lax.rem(bz + offset(s), parts)
        o = lax.rem(mine + d, n_cplx)
        return pltpu.make_async_remote_copy(
            src_ref=sendt_s.at[s],
            dst_ref=recvt_s.at[bz * n_cplx + mine],
            send_sem=sendt_sem.at[s],
            recv_sem=recvt_sem.at[bz],
            device_id=(by * parts + p, o),
            device_id_type=MESH,
        )

    def await_part(zs, count):
        at = recvt_s.at[pl.ds(zs * n_cplx, count)]
        pltpu.make_async_copy(at, at, recvt_sem.at[zs]).wait()
        at = recv_s.at[pl.ds(zs * n_cplx, count)]
        pltpu.make_async_copy(at, at, recv_sem.at[zs]).wait()

    def y_copy(zs, d, small):
        to = lax.rem(by + d, blocks)
        ref, sent, sem = (
            (yrecvt_s, ysendt_sem, yrecvt_sem) if small else (yrecv_s, ysend_sem, yrecv_sem)
        )
        at = pl.ds((by * parts + zs) * slots, slots)
        return pltpu.make_async_remote_copy(
            src_ref=ref.at[at],
            dst_ref=ref.at[at],
            send_sem=sent.at[zs],
            recv_sem=sem.at[by],
            device_id=(to * parts + bz, mine),
            device_id_type=MESH,
        )

    order = sorted(range(1, blocks), key=lambda d: -min(d, blocks - d))

    def forward(s, count):
        zs = lax.rem(bz + parts - offset(s), parts)
        await_part(zs, count)
        from_o = [tab_s[1, zs * slots + j] for j in range(slots)]
        pieces = [jnp.zeros((rows, side), F32)] * slots
        lines = [jnp.zeros((1, rows), F32)] * slots
        for o in range(n_cplx):
            piece = recv_s[zs * n_cplx + o]
            line = recvt_s[zs * n_cplx + o]
            for j in range(slots):
                pieces[j] = jnp.where(from_o[j] == o, piece, pieces[j])
                short = line[:, j * rows : (j + 1) * rows]
                lines[j] = jnp.where(from_o[j] == o, short, lines[j])
        for j in range(slots):
            to = (by * parts + zs) * slots + j
            yrecvt_s[to, :, 0:rows] = lines[j]
            yrecv_s[to] = pieces[j]
        for d in order:
            y_copy(zs, d, True).start()
        for d in order:
            y_copy(zs, d, False).start()

    tab_copy.wait()

    def stage(s, carry):
        @pl.when(s < last)
        def _():
            for j in range(slots):
                x_copy(s + 1, j).wait()

        def body(i, inner):
            g = UNROLL * i
            stop = parts * per_stage - 1
            row = pl.multiple_of(g * GROUP, UNROLL * GROUP)
            for u in range(UNROLL):
                stage_b((u + 1) % 2)
                stage_c(row + u * GROUP, (g + u) // per_slot, u % 2, u % 3)
                stage_a(jnp.minimum(s * per_stage + g + u + 3, stop), (u + 1) % 2, u % 3)
            return inner

        lax.fori_loop(0, per_stage // UNROLL, body, 0)

        p = lax.rem(bz + offset(s), parts)
        start = pl.multiple_of(p * rows, rows)
        errs = []
        for j in range(slots):
            weight = weight_s[j, pl.ds(start, rows), :]
            errs.append(err_s[j * rows : (j + 1) * rows, :] * weight)
            tm_s[j * rows : (j + 1) * rows, :] = tm_s[j * rows : (j + 1) * rows, :] * weight
        sendt_s[s] = jnp.sum(tm_s[...].T, axis=0, keepdims=True)
        for o in range(n_cplx):
            piece = jnp.zeros_like(errs[0])
            for j in range(slots):
                piece = jnp.where(owners[j] == o, errs[j], piece)
            send_s[s, o] = piece

        @pl.when(s == 0)
        def _():
            pl.semaphore_wait(barrier, plane - 1 + blocks - 1)

        for d in range(1, n_cplx):
            tm_copy(s, d).start()
        for d in range(1, n_cplx):
            err_copy(s, d).start()

        @pl.when(s < last)
        def _():
            tm_copy(s, 0).start()
            err_copy(s, 0).start()

        @pl.when(s == last)
        def _():
            recv_s[bz * n_cplx + mine] = send_s[s, mine]
            recvt_s[bz * n_cplx + mine] = sendt_s[s]

        @pl.when(s >= LAG)
        def _():
            forward(s - LAG, n_cplx)

        return carry

    lax.fori_loop(0, parts, stage, 0)
    for s in range(max(parts - LAG, 0), parts):
        forward(s, n_cplx if s < last else n_cplx - 1)

    def y_wait(ref, sem, ys):
        at = ref.at[pl.ds(ys * parts * slots, parts * slots)]
        pltpu.make_async_copy(at, at, sem.at[ys]).wait()

    for d in range(1, blocks):
        y_wait(yrecvt_s, yrecvt_sem, lax.rem(by + d, blocks))

    for q in range(blocks):
        for m in range(cpx_dev):
            acc = jnp.zeros((1, rows), F32)
            for e in range(blocks):
                found = tab_s[0, (q * cpx_dev + m) * blocks + e]
                line = yrecvt_s[jnp.clip(found - 1, 0, blocks * parts * slots - 1)][:, 0:rows]
                acc = acc + jnp.where(found > 0, line, 0.0)
            acc_s[q, m : m + 1, 0:rows] = acc
    top_s[...] = jnp.max(acc_s[...] / den_s[...], axis=0)

    def top_copy(d):
        return pltpu.make_async_remote_copy(
            src_ref=top_s,
            dst_ref=topz_s.at[bz],
            send_sem=topsend_sem.at[d],
            recv_sem=topz_sem.at[bz],
            device_id=(by * parts + lax.rem(bz + d, parts), mine),
            device_id_type=MESH,
        )

    for d in sorted(range(1, parts), key=lambda d: -min(d, parts - d)):
        top_copy(d).start()

    for d in range(1, blocks):
        y_wait(yrecv_s, yrecv_sem, lax.rem(by + d, blocks))
    for m in range(cpx_dev):
        total = jnp.zeros((rows, side), F32)
        for q in range(blocks):
            found = tab_s[0, (by * cpx_dev + m) * blocks + q]
            piece = jnp.where(found > 0, yrecv_s[jnp.clip(found - 1, 0, blocks * parts * slots - 1)], 0.0)
            map_ref[m, :, q * side : (q + 1) * side] = piece
            total = total + piece
        sum_s[m * rows : (m + 1) * rows, :] = total
    totals = jnp.sum(sum_s[...].T, axis=0, keepdims=True)
    for m in range(cpx_dev):
        denom = den_s[by, m : m + 1, 0:rows]
        res_ref[m : m + 1, :] = totals[:, m * rows : (m + 1) * rows] / denom

    best = top_s[...]
    for d in range(1, parts):
        zs = lax.rem(bz + d, parts)
        pltpu.make_async_copy(topz_s.at[zs], topz_s.at[zs], topz_sem.at[zs]).wait()
        best = jnp.maximum(best, topz_s[zs])
    best = jnp.broadcast_to(jnp.max(best, axis=1, keepdims=True), (8, lanes))
    down = lax.broadcasted_iota(jnp.int32, (8, lanes), 0)
    across = lax.broadcasted_iota(jnp.int32, (8, lanes), 1)
    best_ref[...] = jnp.sum(jnp.where(down == across, best, 0.0), axis=0, keepdims=True)

    def drain(s, count):
        at = send_s.at[s, pl.ds(0, count)]
        pltpu.make_async_copy(at, at, send_sem.at[s]).wait()
        at = recvt_s.at[pl.ds(0, count)]
        pltpu.make_async_copy(at, at, sendt_sem.at[s]).wait()

    def drain_all(s, carry):
        drain(s, n_cplx)
        return carry

    lax.fori_loop(0, last, drain_all, 0)
    drain(last, n_cplx - 1)

    def drain_y(zs, carry):
        at = pl.ds(0, (blocks - 1) * slots)
        pltpu.make_async_copy(yrecvt_s.at[at], yrecvt_s.at[at], ysendt_sem.at[zs]).wait()
        pltpu.make_async_copy(yrecv_s.at[at], yrecv_s.at[at], ysend_sem.at[zs]).wait()
        return carry

    lax.fori_loop(0, parts, drain_y, 0)
    for d in range(1, parts):
        top_copy(d).wait_send()


def hand_out(map_in, res_in, best_in, map_ref, res_ref, best_ref):
    map_ref[...] = map_in[...]
    res_ref[...] = res_in[...]
    best_ref[...] = best_in[:, 0 : best_ref.shape[1]]


def shards(pair_tiles, tile_map, lengths, resolved, ln_gain, w_in, w_out, w_head, head_bias):
    n_tile = lax.axis_size("tile")
    n_cplx = lax.axis_size("cplx")
    slots, side, _, chan = pair_tiles.shape
    hid = w_in.shape[1]
    bins = w_head.shape[1]
    complexes, maxres = resolved.shape
    blocks = maxres // side
    cpx_dev = complexes // n_cplx
    rows = maxres // n_tile
    parts = side // rows
    cells = cpx_dev * blocks
    vmem = pl.BlockSpec(memory_space=pltpu.VMEM)
    dma = pltpu.SemaphoreType.DMA
    groups = GROUP * side
    error_map, residue, best = pl.pallas_call(
        functools.partial(fused_kernel, blocks=blocks, parts=parts, n_cplx=n_cplx),
        in_specs=[pl.BlockSpec(memory_space=pl.ANY)] * 9,
        out_specs=[vmem] * 3,
        out_shape=[
            jax.ShapeDtypeStruct((cpx_dev, rows, maxres), F32),
            jax.ShapeDtypeStruct((cpx_dev, rows), F32),
            jax.ShapeDtypeStruct((1, 128), F32),
        ],
        scratch_shapes=[
            pltpu.SMEM((3, tile_map.shape[0]), jnp.int32),
            pltpu.SMEM((complexes,), jnp.int32),
            pltpu.VMEM((3, tile_map.shape[0]), jnp.int32),
            pltpu.VMEM((complexes, maxres), jnp.int32),
            pltpu.VMEM((1, chan), F32),
            pltpu.VMEM((chan, hid), BF16),
            pltpu.VMEM((hid, chan), BF16),
            pltpu.VMEM((bins, chan), BF16),
            pltpu.VMEM((1, bins), F32),
            dma((9,)),
            pltpu.VMEM((chan + bins, chan), BF16),
            pltpu.VMEM((hid, chan), BF16),
            pltpu.VMEM((bins, hid), BF16),
            pltpu.VMEM((bins, 128), F32),
            pltpu.VMEM((bins, 128), F32),
            pltpu.VMEM((slots, bins, 128), F32),
            pltpu.VMEM((slots, side, side), F32),
            pltpu.VMEM((parts * slots * rows, side, chan), BF16),
            pltpu.VMEM((2, chan, groups), BF16),
            pltpu.VMEM((2, hid, groups), BF16),
            pltpu.VMEM((3, bins, groups), F32),
            pltpu.VMEM((3, 1, groups), F32),
            pltpu.VMEM((slots * rows, side), F32),
            pltpu.VMEM((128, side), F32),
            pltpu.VMEM((8, 128), jnp.int32),
            pltpu.SMEM((8, 128), jnp.int32),
            pltpu.VMEM((blocks, 8, 128), F32),
            pltpu.VMEM((blocks, 8, 128), F32),
            pltpu.VMEM((128, side), F32),
            pltpu.VMEM((parts, n_cplx, rows, side), F32),
            pltpu.VMEM((parts, 1, 128), F32),
            pltpu.VMEM((parts * n_cplx, rows, side), F32),
            pltpu.VMEM((parts * n_cplx, 1, 128), F32),
            pltpu.VMEM((blocks * parts * slots, rows, side), F32),
            pltpu.VMEM((blocks * parts * slots, 1, 128), F32),
            pltpu.VMEM((8, 128), F32),
            pltpu.VMEM((parts, 8, 128), F32),
            dma((parts, slots)),
            dma((1,)),
            dma((parts,)),
            dma((parts,)),
            dma((parts,)),
            dma((parts,)),
            dma((parts,)),
            dma((parts,)),
            dma((blocks,)),
            dma((blocks,)),
            dma((parts,)),
            dma((parts,)),
        ],
        compiler_params=pltpu.CompilerParams(
            collective_id=0, has_side_effects=True, vmem_limit_bytes=67043328
        ),
        name="fused",
    )(
        tile_map.T,
        lengths,
        pair_tiles,
        resolved,
        ln_gain.reshape(1, chan),
        w_in,
        w_out,
        w_head.T,
        head_bias.reshape(1, bins),
    )
    error_map, residue, best = pl.pallas_call(
        hand_out,
        in_specs=[vmem] * 3,
        out_specs=[vmem] * 3,
        out_shape=[
            jax.ShapeDtypeStruct(error_map.shape, F32),
            jax.ShapeDtypeStruct(residue.shape, F32),
            jax.ShapeDtypeStruct((1, cpx_dev), F32),
        ],
        name="hand_out",
    )(error_map, residue, best)
    return error_map, residue, best.reshape(cpx_dev)


def solution(mesh):
    placed = (P(("tile", "cplx"), None, None, None), P(), P(), P(), P(), P(), P(), P(), P())
    return jax.shard_map(
        shards,
        mesh=mesh,
        in_specs=placed,
        out_specs=(P("cplx", "tile", None), P("cplx", "tile"), P("cplx")),
        check_vma=False,
    )
```

```python
import functools
import jax
import jax.numpy as jnp
from jax import lax
from jax.experimental import pallas as pl
from jax.experimental.pallas import tpu as pltpu
from jax.sharding import PartitionSpec as P

EPS = 1e-05
LOG2E = 1.4426950408889634
F32 = jnp.float32
BF16 = jnp.bfloat16
MESH = pl.DeviceIdType.MESH
GROUP = 8
LAG = 3
UNROLL = 6


def fused_kernel(
    tmap_h,
    lengths_h,
    x_ref,
    resolved_h,
    gain_h,
    w_in_h,
    w_out_h,
    w_head_h,
    bias_h,
    map_ref,
    res_ref,
    best_ref,
    tmap_ref,
    lengths_ref,
    vmap_ref,
    resolved_ref,
    gain_ref,
    w_in_ref,
    w_out_ref,
    w_head_ref,
    bias_ref,
    in_sem,
    mix_s,
    w1_s,
    w2_s,
    bias_s,
    cen_s,
    tmw_s,
    weight_s,
    x_s,
    xc_s,
    h_s,
    hd_s,
    rs_s,
    err_s,
    tm_s,
    tab_v,
    tab_s,
    den_s,
    acc_s,
    sum_s,
    send_s,
    sendt_s,
    recv_s,
    recvt_s,
    yrecv_s,
    yrecvt_s,
    top_s,
    topz_s,
    x_sem,
    tab_sem,
    send_sem,
    sendt_sem,
    recv_sem,
    recvt_sem,
    ysend_sem,
    ysendt_sem,
    yrecv_sem,
    yrecvt_sem,
    topsend_sem,
    topz_sem,
    *,
    blocks,
    parts,
    n_cplx,
):
    slots, side, _, chan = x_ref.shape
    bins = bias_h.shape[1]
    lanes = 128
    rows = side // parts
    cpx_dev = map_ref.shape[0]
    cells = cpx_dev * blocks
    tile = lax.axis_index("tile")
    mine = lax.axis_index("cplx")
    by = tile // parts
    bz = lax.rem(tile, parts)
    device = tile * n_cplx + mine
    last = parts - 1

    def whole_div(n, d):
        return ((n * (65536 // d + 1)) >> 16) if d > 1 else n

    def offset(s):
        return parts // 2 + (1 - 2 * (s & 1)) * ((s + 1) >> 1)

    def x_copy(s, j):
        p = lax.rem(bz + offset(s), parts)
        return pltpu.make_async_copy(
            x_ref.at[j, pl.ds(p * rows, rows)],
            x_s.at[pl.ds((s * slots + j) * rows, rows)],
            x_sem.at[s, j],
        )

    def x_start(s, carry):
        for j in range(slots):
            x_copy(s, j).start()
        return carry

    def bring(i):
        pairs = (
            (w_head_h, w_head_ref),
            (bias_h, bias_ref),
            (w_in_h, w_in_ref),
            (gain_h, gain_ref),
            (w_out_h, w_out_ref),
            (tmap_h, vmap_ref),
            (tmap_h, tmap_ref),
            (lengths_h, lengths_ref),
            (resolved_h, resolved_ref),
        )
        return pltpu.make_async_copy(*pairs[i], in_sem.at[i])

    bring(0).start()
    for j in range(slots):
        x_copy(0, j).start()
    for i in range(1, 9):
        bring(i).start()
    lax.fori_loop(1, parts, x_start, 0)

    barrier = pltpu.get_barrier_semaphore()
    plane = parts * n_cplx

    for dz in range(parts):
        to = by * parts + lax.rem(bz + dz, parts)
        for d in range(1 if dz == 0 else 0, n_cplx):
            pl.semaphore_signal(
                barrier,
                inc=1,
                device_id=(to, lax.rem(mine + d, n_cplx)),
                device_id_type=MESH,
            )
    for d in range(1, blocks):
        pl.semaphore_signal(
            barrier,
            inc=1,
            device_id=(lax.rem(by + d, blocks) * parts + bz, mine),
            device_id_type=MESH,
        )

    for i in range(9):
        bring(i).wait()
    r = lax.broadcasted_iota(jnp.int32, (chan, chan), 0)
    c = lax.broadcasted_iota(jnp.int32, (chan, chan), 1)
    mix_s[0:chan, :] = (jnp.where(r == c, 1.0, 0.0) - 1.0 / chan).astype(BF16)
    mix_s[chan : chan + bins, :] = w_head_ref[...]
    w1_s[...] = (w_in_ref[...].astype(F32).T * gain_ref[...]).astype(BF16)
    w2_s[...] = lax.dot_general(
        w_head_ref[...], w_out_ref[...], (((1,), (1,)), ((), ())), preferred_element_type=F32
    ).astype(BF16)
    bias_s[...] = jnp.broadcast_to(bias_ref[...] * LOG2E, (lanes, bins)).T
    b = lax.broadcasted_iota(jnp.int32, (bins, lanes), 0).astype(F32)
    cen_s[...] = (b + 0.5) * (31.0 / (bins - 2))
    pos = lax.broadcasted_iota(jnp.int32, (1, side), 1)

    def stage_a(group, par, keep):
        row = pl.multiple_of(group * GROUP, GROUP)
        x = x_s[pl.ds(row, GROUP), :, :].reshape(GROUP * side, chan)
        first = lax.dot_general(
            mix_s[...], x, (((1,), (1,)), ((), ())), preferred_element_type=F32
        )
        xc = first[:chan]
        var = jnp.mean(xc * xc, axis=0, keepdims=True)
        xc_s[par] = xc.astype(BF16)
        rs_s[keep] = lax.rsqrt(var + EPS) * LOG2E
        bias = jnp.concatenate([bias_s[...]] * GROUP, axis=1)
        hd_s[keep] = first[chan:] * LOG2E + bias

    def stage_b(par):
        z = jnp.dot(w1_s[...], xc_s[par], preferred_element_type=F32)
        h_s[par] = jnp.maximum(z, 0.0).astype(BF16)

    def stage_c(row, slot, par, keep):
        cen = jnp.concatenate([cen_s[...]] * GROUP, axis=1)
        tmw = jnp.concatenate([tmw_s[slot]] * GROUP, axis=1)
        y = jnp.dot(w2_s[...], h_s[par], preferred_element_type=F32)
        logits = hd_s[keep] + rs_s[keep] * y
        top = jnp.max(logits, axis=0, keepdims=True)
        e = jnp.exp2(logits - top)
        s0 = jnp.sum(e, axis=0, keepdims=True)
        s1 = jnp.sum(e * cen, axis=0, keepdims=True)
        s2 = jnp.sum(e * tmw, axis=0, keepdims=True)
        inv = 1.0 / s0
        expected = s1 * inv
        term = s2 * inv
        for i in range(GROUP):
            err_s[pl.ds(row + i, 1), :] = expected[:, i * side : (i + 1) * side]
            tm_s[pl.ds(row + i, 1), :] = term[:, i * side : (i + 1) * side]

    n = lax.broadcasted_iota(jnp.int32, (1, vmap_ref.shape[1]), 1)
    unit = whole_div(n, slots)
    slot_of = n - unit * slots
    tile_of = whole_div(unit, n_cplx)
    cplx_of = unit - tile_of * n_cplx
    k_all = vmap_ref[0:1, :]
    member = k_all - mine * cpx_dev
    here = (k_all >= 0) & (member >= 0) & (member < cpx_dev)
    key = jnp.where(here, (vmap_ref[1:2, :] * cpx_dev + member) * blocks + vmap_ref[2:3, :], -1)
    near = tile_of - by * parts
    key2 = jnp.where(here & (near >= 0) & (near < parts), near * slots + slot_of, -1)
    want = lax.broadcasted_iota(jnp.int32, (128, n.shape[1]), 0)
    spot = jnp.where(want == key, tile_of * slots + slot_of + 1, 0)
    spot2 = jnp.where(want == key2, cplx_of, 0)
    tab_v[...] = jnp.zeros_like(tab_v)
    for i, wide in enumerate((spot, spot2)):
        folded = jnp.zeros((128, 128), jnp.int32)
        width = wide.shape[1]
        for at in range(0, width, 128):
            piece = wide[:, at : min(at + 128, width)]
            if piece.shape[1] < 128:
                fill = jnp.zeros((128, 128 - piece.shape[1]), jnp.int32)
                piece = jnp.concatenate([piece, fill], axis=1)
            folded = folded + piece
        folded = folded.T
        while folded.shape[0] > 1:
            half = folded.shape[0] // 2
            folded = folded[:half] + folded[half:]
        tab_v[i : i + 1, :] = folded
    tab_copy = pltpu.make_async_copy(tab_v, tab_s, tab_sem.at[0])
    tab_copy.start()

    x_copy(0, 0).wait()
    stage_a(0, 0, 0)
    stage_a(1, 1, 1)
    for j in range(1, slots):
        x_copy(0, j).wait()
    stage_b(0)
    stage_a(2, 0, 2)

    def valid(k, length, block):
        line = resolved_ref[pl.ds(k, 1), :]
        part = jnp.zeros((1, side), jnp.int32)
        for q in range(blocks):
            part = jnp.where(block == q, line[:, q * side : (q + 1) * side], part)
        return jnp.where((pos + block * side < length) & (part > 0), 1.0, 0.0)

    owners = []
    for j in range(slots):
        at = device * slots + j
        found = tmap_ref[0, at]
        k = jnp.maximum(found, 0)
        length = lengths_ref[k]
        size = jnp.full((bins, lanes), jnp.maximum(length, 19).astype(F32) - 15.0, F32)
        d0 = 1.24 * jnp.exp(jnp.log(size) * (1.0 / 3.0)) - 1.8
        ratio = cen_s[...] / d0
        tmw_s[j] = 1.0 / (1.0 + ratio * ratio)
        row_valid = valid(k, length, jnp.maximum(tmap_ref[1, at], 0))
        col_valid = valid(k, length, jnp.maximum(tmap_ref[2, at], 0))
        col_valid = jnp.where(found >= 0, col_valid, 0.0)
        weight_s[j] = jnp.broadcast_to(row_valid, (side, side)).T * col_valid
        owners.append(jnp.where(found >= 0, whole_div(k, cpx_dev), -1))

    acc_s[...] = jnp.zeros_like(acc_s)
    den_s[...] = jnp.ones_like(den_s)
    for m in range(cpx_dev):
        k = mine * cpx_dev + m
        length = lengths_ref[k]
        line = resolved_ref[pl.ds(k, 1), :]
        where = lax.broadcasted_iota(jnp.int32, line.shape, 1)
        valid_line = jnp.where((where < length) & (line > 0), 1.0, 0.0)
        total = jnp.sum(valid_line, axis=1, keepdims=True)
        for q in range(blocks):
            part = valid_line[:, q * side : (q + 1) * side]
            own = pltpu.roll(part, lax.rem(side - bz * rows, side), 1)
            den_s[q, m : m + 1, :] = jnp.maximum(own * total, 1.0)

    per_stage = slots * rows // GROUP
    per_slot = rows // GROUP
    tm_s[...] = jnp.zeros_like(tm_s)

    def err_copy(s, d):
        p = lax.rem(bz + offset(s), parts)
        o = lax.rem(mine + d, n_cplx)
        return pltpu.make_async_remote_copy(
            src_ref=send_s.at[s, o],
            dst_ref=recv_s.at[bz * n_cplx + mine],
            send_sem=send_sem.at[s],
            recv_sem=recv_sem.at[bz],
            device_id=(by * parts + p, o),
            device_id_type=MESH,
        )

    def tm_copy(s, d):
        p = lax.rem(bz + offset(s), parts)
        o = lax.rem(mine + d, n_cplx)
        return pltpu.make_async_remote_copy(
            src_ref=sendt_s.at[s],
            dst_ref=recvt_s.at[bz * n_cplx + mine],
            send_sem=sendt_sem.at[s],
            recv_sem=recvt_sem.at[bz],
            device_id=(by * parts + p, o),
            device_id_type=MESH,
        )

    def y_copy(zs, d, small):
        to = lax.rem(by + d, blocks)
        ref, sent, sem = (
            (yrecvt_s, ysendt_sem, yrecvt_sem) if small else (yrecv_s, ysend_sem, yrecv_sem)
        )
        at = pl.ds((by * parts + zs) * slots, slots)
        return pltpu.make_async_remote_copy(
            src_ref=ref.at[at],
            dst_ref=ref.at[at],
            send_sem=sent.at[zs],
            recv_sem=sem.at[by],
            device_id=(to * parts + bz, mine),
            device_id_type=MESH,
        )

    order = sorted(range(1, blocks), key=lambda d: -min(d, blocks - d))

    def forward_tm(s, count):
        zs = lax.rem(bz + parts - offset(s), parts)
        at = recvt_s.at[pl.ds(zs * n_cplx, count)]
        pltpu.make_async_copy(at, at, recvt_sem.at[zs]).wait()
        lines = [jnp.zeros((1, rows), F32)] * slots
        for o in range(n_cplx):
            line = recvt_s[zs * n_cplx + o]
            for j in range(slots):
                short = line[:, j * rows : (j + 1) * rows]
                lines[j] = jnp.where(tab_s[1, zs * slots + j] == o, short, lines[j])
        for j in range(slots):
            yrecvt_s[(by * parts + zs) * slots + j, :, 0:rows] = lines[j]
        for d in order:
            y_copy(zs, d, True).start()

    def forward_err(s, count):
        zs = lax.rem(bz + parts - offset(s), parts)
        at = recv_s.at[pl.ds(zs * n_cplx, count)]
        pltpu.make_async_copy(at, at, recv_sem.at[zs]).wait()
        pieces = [jnp.zeros((rows, side), F32)] * slots
        for o in range(n_cplx):
            piece = recv_s[zs * n_cplx + o]
            for j in range(slots):
                pieces[j] = jnp.where(tab_s[1, zs * slots + j] == o, piece, pieces[j])
        for j in range(slots):
            yrecv_s[(by * parts + zs) * slots + j] = pieces[j]
        for d in order:
            y_copy(zs, d, False).start()

    def forward(s, count):
        forward_tm(s, count)
        forward_err(s, count)

    tab_copy.wait()

    def stage(s, carry):
        @pl.when(s < last)
        def _():
            for j in range(slots):
                x_copy(s + 1, j).wait()

        def body(i, inner):
            g = UNROLL * i
            stop = parts * per_stage - 1
            row = pl.multiple_of(g * GROUP, UNROLL * GROUP)
            for u in range(UNROLL):
                stage_b((u + 1) % 2)
                stage_c(row + u * GROUP, (g + u) // per_slot, u % 2, u % 3)
                stage_a(jnp.minimum(s * per_stage + g + u + 3, stop), (u + 1) % 2, u % 3)
            return inner

        lax.fori_loop(0, per_stage // UNROLL, body, 0)

        p = lax.rem(bz + offset(s), parts)
        start = pl.multiple_of(p * rows, rows)
        errs = []
        for j in range(slots):
            weight = weight_s[j, pl.ds(start, rows), :]
            errs.append(err_s[j * rows : (j + 1) * rows, :] * weight)
            tm_s[j * rows : (j + 1) * rows, :] = tm_s[j * rows : (j + 1) * rows, :] * weight
        sendt_s[s] = jnp.sum(tm_s[...].T, axis=0, keepdims=True)
        for o in range(n_cplx):
            piece = jnp.zeros_like(errs[0])
            for j in range(slots):
                piece = jnp.where(owners[j] == o, errs[j], piece)
            send_s[s, o] = piece

        @pl.when(s == 0)
        def _():
            pl.semaphore_wait(barrier, plane - 1 + blocks - 1)

        for d in range(1, n_cplx):
            tm_copy(s, d).start()
        for d in range(1, n_cplx):
            err_copy(s, d).start()

        @pl.when(s < last)
        def _():
            tm_copy(s, 0).start()
            err_copy(s, 0).start()

        @pl.when(s == last)
        def _():
            recv_s[bz * n_cplx + mine] = send_s[s, mine]
            recvt_s[bz * n_cplx + mine] = sendt_s[s]

        @pl.when(s >= LAG)
        def _():
            forward(s - LAG, n_cplx)

        return carry

    lax.fori_loop(0, parts, stage, 0)
    for s in range(max(parts - LAG, 0), parts):
        forward(s, n_cplx if s < last else n_cplx - 1)

    def y_wait(ref, sem, ys):
        at = ref.at[pl.ds(ys * parts * slots, parts * slots)]
        pltpu.make_async_copy(at, at, sem.at[ys]).wait()

    for d in range(1, blocks):
        y_wait(yrecvt_s, yrecvt_sem, lax.rem(by + d, blocks))

    for q in range(blocks):
        for m in range(cpx_dev):
            acc = jnp.zeros((1, rows), F32)
            for e in range(blocks):
                found = tab_s[0, (q * cpx_dev + m) * blocks + e]
                line = yrecvt_s[jnp.clip(found - 1, 0, blocks * parts * slots - 1)][:, 0:rows]
                acc = acc + jnp.where(found > 0, line, 0.0)
            acc_s[q, m : m + 1, 0:rows] = acc
    top_s[...] = jnp.max(acc_s[...] / den_s[...], axis=0)

    def top_copy(d):
        return pltpu.make_async_remote_copy(
            src_ref=top_s,
            dst_ref=topz_s.at[bz],
            send_sem=topsend_sem.at[d],
            recv_sem=topz_sem.at[bz],
            device_id=(by * parts + lax.rem(bz + d, parts), mine),
            device_id_type=MESH,
        )

    for d in sorted(range(1, parts), key=lambda d: -min(d, parts - d)):
        top_copy(d).start()

    for d in range(1, blocks):
        y_wait(yrecv_s, yrecv_sem, lax.rem(by + d, blocks))
    for m in range(cpx_dev):
        total = jnp.zeros((rows, side), F32)
        for q in range(blocks):
            found = tab_s[0, (by * cpx_dev + m) * blocks + q]
            piece = jnp.where(found > 0, yrecv_s[jnp.clip(found - 1, 0, blocks * parts * slots - 1)], 0.0)
            map_ref[m, :, q * side : (q + 1) * side] = piece
            total = total + piece
        sum_s[m * rows : (m + 1) * rows, :] = total
    totals = jnp.sum(sum_s[...].T, axis=0, keepdims=True)
    for m in range(cpx_dev):
        denom = den_s[by, m : m + 1, 0:rows]
        res_ref[m : m + 1, :] = totals[:, m * rows : (m + 1) * rows] / denom

    best = top_s[...]
    for d in range(1, parts):
        zs = lax.rem(bz + d, parts)
        pltpu.make_async_copy(topz_s.at[zs], topz_s.at[zs], topz_sem.at[zs]).wait()
        best = jnp.maximum(best, topz_s[zs])
    best = jnp.broadcast_to(jnp.max(best, axis=1, keepdims=True), (8, lanes))
    down = lax.broadcasted_iota(jnp.int32, (8, lanes), 0)
    across = lax.broadcasted_iota(jnp.int32, (8, lanes), 1)
    best_ref[...] = jnp.sum(jnp.where(down == across, best, 0.0), axis=0, keepdims=True)

    def drain(s, count):
        at = send_s.at[s, pl.ds(0, count)]
        pltpu.make_async_copy(at, at, send_sem.at[s]).wait()
        at = recvt_s.at[pl.ds(0, count)]
        pltpu.make_async_copy(at, at, sendt_sem.at[s]).wait()

    def drain_all(s, carry):
        drain(s, n_cplx)
        return carry

    lax.fori_loop(0, last, drain_all, 0)
    drain(last, n_cplx - 1)

    def drain_y(zs, carry):
        at = pl.ds(0, (blocks - 1) * slots)
        pltpu.make_async_copy(yrecvt_s.at[at], yrecvt_s.at[at], ysendt_sem.at[zs]).wait()
        pltpu.make_async_copy(yrecv_s.at[at], yrecv_s.at[at], ysend_sem.at[zs]).wait()
        return carry

    lax.fori_loop(0, parts, drain_y, 0)
    for d in range(1, parts):
        top_copy(d).wait_send()


def hand_out(map_in, res_in, best_in, map_ref, res_ref, best_ref):
    map_ref[...] = map_in[...]
    res_ref[...] = res_in[...]
    best_ref[...] = best_in[:, 0 : best_ref.shape[1]]


def shards(pair_tiles, tile_map, lengths, resolved, ln_gain, w_in, w_out, w_head, head_bias):
    n_tile = lax.axis_size("tile")
    n_cplx = lax.axis_size("cplx")
    slots, side, _, chan = pair_tiles.shape
    hid = w_in.shape[1]
    bins = w_head.shape[1]
    complexes, maxres = resolved.shape
    blocks = maxres // side
    cpx_dev = complexes // n_cplx
    rows = maxres // n_tile
    parts = side // rows
    cells = cpx_dev * blocks
    vmem = pl.BlockSpec(memory_space=pltpu.VMEM)
    dma = pltpu.SemaphoreType.DMA
    groups = GROUP * side
    error_map, residue, best = pl.pallas_call(
        functools.partial(fused_kernel, blocks=blocks, parts=parts, n_cplx=n_cplx),
        in_specs=[pl.BlockSpec(memory_space=pl.ANY)] * 9,
        out_specs=[vmem] * 3,
        out_shape=[
            jax.ShapeDtypeStruct((cpx_dev, rows, maxres), F32),
            jax.ShapeDtypeStruct((cpx_dev, rows), F32),
            jax.ShapeDtypeStruct((1, 128), F32),
        ],
        scratch_shapes=[
            pltpu.SMEM((3, tile_map.shape[0]), jnp.int32),
            pltpu.SMEM((complexes,), jnp.int32),
            pltpu.VMEM((3, tile_map.shape[0]), jnp.int32),
            pltpu.VMEM((complexes, maxres), jnp.int32),
            pltpu.VMEM((1, chan), F32),
            pltpu.VMEM((chan, hid), BF16),
            pltpu.VMEM((hid, chan), BF16),
            pltpu.VMEM((bins, chan), BF16),
            pltpu.VMEM((1, bins), F32),
            dma((9,)),
            pltpu.VMEM((chan + bins, chan), BF16),
            pltpu.VMEM((hid, chan), BF16),
            pltpu.VMEM((bins, hid), BF16),
            pltpu.VMEM((bins, 128), F32),
            pltpu.VMEM((bins, 128), F32),
            pltpu.VMEM((slots, bins, 128), F32),
            pltpu.VMEM((slots, side, side), F32),
            pltpu.VMEM((parts * slots * rows, side, chan), BF16),
            pltpu.VMEM((2, chan, groups), BF16),
            pltpu.VMEM((2, hid, groups), BF16),
            pltpu.VMEM((3, bins, groups), F32),
            pltpu.VMEM((3, 1, groups), F32),
            pltpu.VMEM((slots * rows, side), F32),
            pltpu.VMEM((128, side), F32),
            pltpu.VMEM((8, 128), jnp.int32),
            pltpu.SMEM((8, 128), jnp.int32),
            pltpu.VMEM((blocks, 8, 128), F32),
            pltpu.VMEM((blocks, 8, 128), F32),
            pltpu.VMEM((128, side), F32),
            pltpu.VMEM((parts, n_cplx, rows, side), F32),
            pltpu.VMEM((parts, 1, 128), F32),
            pltpu.VMEM((parts * n_cplx, rows, side), F32),
            pltpu.VMEM((parts * n_cplx, 1, 128), F32),
            pltpu.VMEM((blocks * parts * slots, rows, side), F32),
            pltpu.VMEM((blocks * parts * slots, 1, 128), F32),
            pltpu.VMEM((8, 128), F32),
            pltpu.VMEM((parts, 8, 128), F32),
            dma((parts, slots)),
            dma((1,)),
            dma((parts,)),
            dma((parts,)),
            dma((parts,)),
            dma((parts,)),
            dma((parts,)),
            dma((parts,)),
            dma((blocks,)),
            dma((blocks,)),
            dma((parts,)),
            dma((parts,)),
        ],
        compiler_params=pltpu.CompilerParams(
            collective_id=0, has_side_effects=True, vmem_limit_bytes=67043328
        ),
        name="fused",
    )(
        tile_map.T,
        lengths,
        pair_tiles,
        resolved,
        ln_gain.reshape(1, chan),
        w_in,
        w_out,
        w_head.T,
        head_bias.reshape(1, bins),
    )
    error_map, residue, best = pl.pallas_call(
        hand_out,
        in_specs=[vmem] * 3,
        out_specs=[vmem] * 3,
        out_shape=[
            jax.ShapeDtypeStruct(error_map.shape, F32),
            jax.ShapeDtypeStruct(residue.shape, F32),
            jax.ShapeDtypeStruct((1, cpx_dev), F32),
        ],
        name="hand_out",
    )(error_map, residue, best)
    return error_map, residue, best.reshape(cpx_dev)


def solution(mesh):
    placed = (P(("tile", "cplx"), None, None, None), P(), P(), P(), P(), P(), P(), P(), P())
    return jax.shard_map(
        shards,
        mesh=mesh,
        in_specs=placed,
        out_specs=(P("cplx", "tile", None), P("cplx", "tile"), P("cplx")),
        check_vma=False,
    )
```
